128 devices in a mesh: batch: 8 (over x, core), rows: 16 (over z, y).
Axes of the slice: x: 4, y: 4, z: 4, core: 2. Of those that a mesh axis runs over, the one named last changes fastest.
Arguments:
- feat_quarter: bfloat16 [8, 256, 512, 256], P('batch', 'rows'), may hold values from -12 to 12
- feat_eighth: bfloat16 [8, 128, 256, 256], P('batch', 'rows'), may hold values from -12 to 12
- feat_sixteenth: bfloat16 [8, 64, 128, 256], P('batch', 'rows'), may hold values from -12 to 12
- feat_thirty: bfloat16 [8, 32, 64, 256], P('batch', 'rows'), may hold values from -12 to 12
- labels: int32 [8, 256, 512], P('batch', 'rows'), may hold values from 0 to 255, as said below
- first_weights: bfloat16 [4, 3, 3, 256, 128], replicated, may hold values from -0.125 to 0.125
- inner_weights: bfloat16 [3, 3, 3, 128, 128], replicated, may hold values from -0.1875 to 0.1875
- norm_gain: float32 [7, 128], replicated, may hold values from 0.1 to 1.9
- norm_shift: float32 [7, 128], replicated, may hold values from -3 to 3
- class_weight: bfloat16 [128, 19], replicated, may hold values from -0.5 to 0.5
- class_bias: float32 [19], replicated, may hold values from -3 to 3
Outputs:
- logits: bfloat16 [8, 19, 256, 512], P('batch', None, 'rows')
- mean_loss: float32 [], replicated
The draws below stay inside these ranges and needn't reach their ends.
Inputs may be any that keep to these rules, and one draw needn't show every extreme that they name: `labels`: values 0 to 18 name classes; 255 marks a pixel without a label.
All inputs are finite; a program needn't handle non-finite values.
Results may differ from the reference program's by a relative error of at most 0.008.
Values may be sent and summed in bfloat16 or wider, within the bound.
No kernel may reach another device: no remote copies, remote signals or barrier semaphores. Data moves between devices by JAX's collectives and lax.ppermute only.
A program may use at most 128 MiB of HBM per device.

```python
import jax
import jax.numpy as jnp
from jax import lax

C_IN = 256
HEAD = 128
CLASSES = 19
GROUPS = 32
COLS4 = 512
IMAGES = 8
QUARTER_ROWS = 256


def feature_map(key, row_count, col_count, marker):
    level_key = jax.random.fold_in(key, marker)
    base_key, offset_key, slope_key = jax.random.split(level_key, 3)
    array_shape = (IMAGES, row_count, col_count, C_IN)
    row_ramp = ((jnp.arange(row_count, dtype=jnp.float32) + 0.5) / row_count)[None, :, None, None]
    base = jax.random.normal(base_key, array_shape, jnp.float32)
    slope_rate = jax.random.uniform(slope_key, (IMAGES, 1, 1, 1), jnp.float32, 1.0, 1.6)
    offset = jax.random.normal(offset_key, (IMAGES, 1, 1, C_IN), jnp.float32) * 0.5
    row_scale = jnp.exp(1.4 * slope_rate * (row_ramp - 0.5))
    values = base * row_scale + 2.0 * offset * row_ramp
    return jnp.clip(values, -12.0, 12.0).astype(jnp.bfloat16)


def draw_feat_quarter(key, part):
    return feature_map(key, QUARTER_ROWS, COLS4, 11)


def draw_feat_eighth(key, part):
    return feature_map(key, QUARTER_ROWS // 2, COLS4 // 2, 12)


def draw_feat_sixteenth(key, part):
    return feature_map(key, QUARTER_ROWS // 4, COLS4 // 4, 13)


def draw_feat_thirty(key, part):
    return feature_map(key, QUARTER_ROWS // 8, COLS4 // 8, 14)


def draw_labels(key, part):
    class_key, drop_key, major_key, choose_key = jax.random.split(jax.random.fold_in(key, 7), 4)
    array_shape = (IMAGES, QUARTER_ROWS, COLS4)
    classes = jax.random.randint(class_key, array_shape, 0, CLASSES)
    majors = jax.random.randint(major_key, (IMAGES, QUARTER_ROWS // 8), 0, CLASSES)
    row_index = jnp.arange(QUARTER_ROWS, dtype=jnp.int32)
    block_major = majors[:, row_index // 8][:, :, None]
    choose = jax.random.randint(choose_key, array_shape, 0, 1000)
    classes = jnp.where(choose < 700, block_major, classes)
    chance = jax.random.randint(drop_key, array_shape, 0, 1000)
    drop_limit = 40 + 700 * row_index * row_index // (QUARTER_ROWS * QUARTER_ROWS)
    return jnp.where(chance < drop_limit[None, :, None], 255, classes).astype(jnp.int32)


def centred(key, dims, scale, bound, held_as=jnp.bfloat16):
    drawn = jax.random.normal(key, dims, jnp.float32) * scale
    return jnp.minimum(jnp.maximum(drawn, -bound), bound).astype(held_as)


def setup_inputs(seed: int = 0) -> dict:
    arg_keys = jax.random.split(jax.random.key(seed), 12)
    feat_quarter = draw_feat_quarter(jax.random.fold_in(arg_keys[11], 71), 0)
    feat_eighth = draw_feat_eighth(jax.random.fold_in(arg_keys[11], 71), 0)
    feat_sixteenth = draw_feat_sixteenth(jax.random.fold_in(arg_keys[11], 71), 0)
    feat_thirty = draw_feat_thirty(jax.random.fold_in(arg_keys[11], 71), 0)
    labels = draw_labels(jax.random.fold_in(arg_keys[11], 71), 0)
    first_weights = centred(arg_keys[5], (4, 3, 3, C_IN, HEAD), (9 * C_IN) ** -0.5, 0.125)
    inner_weights = centred(arg_keys[6], (3, 3, 3, HEAD, HEAD), (9 * HEAD) ** -0.5, 0.1875)
    norm_gain = jnp.clip(1.0 + 0.18 * jax.random.normal(arg_keys[7], (7, HEAD), jnp.float32), 0.1, 1.9)
    norm_shift = centred(arg_keys[8], (7, HEAD), 0.5, 3.0, jnp.float32)
    class_weight = centred(arg_keys[9], (HEAD, CLASSES), HEAD ** -0.5, 0.5)
    class_bias = centred(arg_keys[10], (CLASSES,), 0.5, 3.0, jnp.float32)
    return {"feat_quarter": feat_quarter, "feat_eighth": feat_eighth, "feat_sixteenth": feat_sixteenth, "feat_thirty": feat_thirty, "labels": labels, "first_weights": first_weights, "inner_weights": inner_weights, "norm_gain": norm_gain, "norm_shift": norm_shift, "class_weight": class_weight, "class_bias": class_bias}


NORM_FLOOR = 0.05

def conv_rows(framed, weight):
    row_count = framed.shape[0] - 2
    col_count = framed.shape[1]
    padded = jnp.pad(framed, ((0, 0), (1, 1), (0, 0)))
    result = jnp.zeros((row_count, col_count, weight.shape[3]), jnp.float32)
    for downward in range(3):
        for across in range(3):
            window = padded[downward:downward + row_count, across:across + col_count, :]
            result = result + jnp.einsum('rwc,cd->rwd', window.astype(jnp.float32), weight[downward, across].astype(jnp.float32))
    return result

def heighten(padded):
    row_count = padded.shape[0] - 2
    middle = padded[1:-1]
    even_rows = 0.75 * middle + 0.25 * padded[:-2]
    odd_rows = 0.75 * middle + 0.25 * padded[2:]
    inner_rows = jnp.stack([even_rows, odd_rows], axis=1).reshape(2 * row_count, padded.shape[1], padded.shape[2])
    upper_row = 0.75 * padded[0] + 0.25 * padded[1]
    lower_row = 0.75 * padded[-1] + 0.25 * padded[-2]
    return jnp.concatenate([upper_row[None], inner_rows, lower_row[None]], axis=0)

def widen(field):
    left_side = jnp.concatenate([field[:, :1], field[:, :-1]], axis=1)
    right_side = jnp.concatenate([field[:, 1:], field[:, -1:]], axis=1)
    even_cols = 0.75 * field + 0.25 * left_side
    odd_cols = 0.75 * field + 0.25 * right_side
    return jnp.stack([even_cols, odd_cols], axis=2).reshape(field.shape[0], 2 * field.shape[1], field.shape[2])

def group_sum(values):
    channel_sums = lax.optimization_barrier(jnp.sum(values, axis=(0, 1)))
    return channel_sums.reshape(GROUPS, -1).sum(axis=1)

def spread(values, width):
    return jnp.repeat(values, width // GROUPS)

def finish(values, group_mean, group_var, gain, shift):
    width = values.shape[2]
    factor = gain * lax.rsqrt(spread(group_var, width) + NORM_FLOOR)
    return jnp.maximum((values - spread(group_mean, width)) * factor + shift, 0.0).astype(jnp.bfloat16)

def normalize(values, gain, shift):
    pixels = values.shape[0] * values.shape[1] * (values.shape[2] // GROUPS)
    group_mean = group_sum(values) / pixels
    centered = values - spread(group_mean, values.shape[2])
    group_var = group_sum(centered * centered) / pixels
    return finish(values, group_mean, group_var, gain, shift)

def upsample(active):
    padded = jnp.pad(active, ((1, 1), (0, 0), (0, 0)), mode='edge').astype(jnp.float32)
    return widen(heighten(padded)[1:-1]).astype(jnp.bfloat16)

def reference(feat_quarter, feat_eighth, feat_sixteenth, feat_thirty, labels, first_weights, inner_weights, norm_gain, norm_shift, class_weight, class_bias):

    def section(image_in, weight, layer_index):
        framed = jnp.pad(image_in, ((1, 1), (0, 0), (0, 0)))
        return normalize(conv_rows(framed, weight), norm_gain[layer_index], norm_shift[layer_index])

    def one_image(image_items):
        quarter_in, eighth_in, sixteenth_in, thirty_in, label_map = image_items
        quarter = section(quarter_in, first_weights[0], 0)
        eighth = upsample(section(eighth_in, first_weights[1], 1))
        sixteenth = upsample(section(upsample(section(sixteenth_in, first_weights[2], 2)), inner_weights[0], 4))
        coarse = upsample(section(thirty_in, first_weights[3], 3))
        thirty = upsample(section(upsample(section(coarse, inner_weights[1], 5)), inner_weights[2], 6))
        combined = (quarter.astype(jnp.float32) + eighth.astype(jnp.float32) + sixteenth.astype(jnp.float32) + thirty.astype(jnp.float32)).astype(jnp.bfloat16)
        scores = jnp.einsum('rwc,ck->krw', combined.astype(jnp.float32), class_weight.astype(jnp.float32)) + class_bias.astype(jnp.float32)[:, None, None]
        log_total = jnp.log(lax.optimization_barrier(jnp.sum(jnp.exp(scores), axis=0)))
        classes = jnp.arange(scores.shape[0], dtype=jnp.int32)[:, None, None]
        picked = lax.optimization_barrier(jnp.sum(jnp.where(classes == label_map[None], scores, 0.0), axis=0))
        usable = label_map != 255
        loss_total = jnp.sum(jnp.where(usable, log_total - picked, 0.0))
        valid_count = jnp.sum(usable.astype(jnp.float32))
        return (scores.astype(jnp.bfloat16), loss_total, valid_count)
    logits, totals, counts = lax.map(one_image, (feat_quarter, feat_eighth, feat_sixteenth, feat_thirty, labels))
    mean_loss = jnp.sum(totals) / jnp.maximum(jnp.sum(counts), 1.0)
    return (logits, mean_loss)
```

```python
import jax
import jax.numpy as jnp
from jax import lax
from jax.sharding import Mesh
from jax.sharding import PartitionSpec as P

GROUPS = 32
ROWS = ("rows_0", "rows_1")
EVERY = ("batch_0", "batch_1", "rows_0", "rows_1")
BATCH = ("batch_0", "batch_1")
NORM_FLOOR = 0.05


def everyone(array, axes, count):
    return lax.all_to_all(jnp.broadcast_to(array[None], (count,) + array.shape), axes, 0, 0)


def conv_rows(framed, weight):
    row_count = framed.shape[0] - 2
    col_count = framed.shape[1]
    padded = jnp.pad(framed, ((0, 0), (1, 1), (0, 0)))
    result = jnp.zeros((row_count, col_count, weight.shape[3]), jnp.float32)
    for downward in range(3):
        for across in range(3):
            window = padded[downward : downward + row_count, across : across + col_count, :]
            result = result + jnp.einsum(
                "rwc,cd->rwd", window, weight[downward, across], preferred_element_type=jnp.float32
            )
    return result


def heighten(padded):
    row_count = padded.shape[0] - 2
    middle = padded[1:-1]
    even_rows = 0.75 * middle + 0.25 * padded[:-2]
    odd_rows = 0.75 * middle + 0.25 * padded[2:]
    return jnp.stack([even_rows, odd_rows], axis=1).reshape(
        2 * row_count, padded.shape[1], padded.shape[2]
    )


def widen(field):
    left_side = jnp.concatenate([field[:, :1], field[:, :-1]], axis=1)
    right_side = jnp.concatenate([field[:, 1:], field[:, -1:]], axis=1)
    even_cols = 0.75 * field + 0.25 * left_side
    odd_cols = 0.75 * field + 0.25 * right_side
    return jnp.stack([even_cols, odd_cols], axis=2).reshape(
        field.shape[0], 2 * field.shape[1], field.shape[2]
    )


def local_stats(values):
    total = jnp.sum(values, axis=(0, 1))
    centred = values - total / (values.shape[0] * values.shape[1])
    return jnp.stack([total, jnp.sum(centred * centred, axis=(0, 1))])


def merged(stats, pixels, gain, shift):
    members, _, width = stats.shape
    per = width // GROUPS
    count = members * pixels * per
    means = stats[:, 0] / pixels
    group_mean = stats[:, 0].reshape(members, GROUPS, per).sum(axis=(0, 2)) / count
    spread_mean = jnp.repeat(group_mean, per)
    square = stats[:, 1] + pixels * jnp.square(means - spread_mean)
    group_var = square.reshape(members, GROUPS, per).sum(axis=(0, 2)) / count
    factor = gain * lax.rsqrt(jnp.repeat(group_var, per) + NORM_FLOOR)
    return spread_mean, factor, shift


def act(values, norm):
    mean, factor, shift = norm
    return jnp.maximum((values - mean) * factor + shift, 0.0).astype(jnp.bfloat16)


def per_device(
    feat_quarter,
    feat_eighth,
    feat_sixteenth,
    feat_thirty,
    labels,
    first_weights,
    inner_weights,
    norm_gain,
    norm_shift,
    class_weight,
    class_bias,
):
    position = lax.axis_index(ROWS)
    bands = lax.axis_size(ROWS)
    first, last = position == 0, position == bands - 1
    up_pairs = [(i, i + 1) for i in range(bands - 1)]
    down_pairs = [(j, i) for i, j in up_pairs]
    feats = [feat_quarter[0], feat_eighth[0], feat_sixteenth[0], feat_thirty[0]]
    depths = [1, 2, 3, 1]
    width = feats[0].shape[2]

    def packed(ends):
        return jnp.concatenate([end.reshape(-1, width) for end in ends])

    before = lax.ppermute(packed([f[-d:] for f, d in zip(feats, depths)]), ROWS, up_pairs)
    after = lax.ppermute(packed([f[:d] for f, d in zip(feats, depths)]), ROWS, down_pairs)
    fields, at = [], 0
    for level, (feat, depth) in enumerate(zip(feats, depths)):
        cols = feat.shape[1]
        size = depth * cols
        shape = (depth, cols, width)
        framed = jnp.concatenate(
            [before[at : at + size].reshape(shape), feat, after[at : at + size].reshape(shape)]
        )
        fields.append(conv_rows(framed, first_weights[level]))
        at += size
    own = [f.shape[0] for f in feats]
    inner = [field[d - 1 : d - 1 + n] for field, d, n in zip(fields, depths, own)]
    stats = jnp.stack([local_stats(inner[level]) for level in range(3)]).reshape(6, -1)
    coarse_shape = inner[3].shape
    head = stats.shape[1]
    got = everyone(jnp.concatenate([stats, inner[3].reshape(-1, head)]), ROWS, bands)
    got_stats = got[:, :6].reshape(bands, 3, 2, head)
    coarse = got[:, 6:].reshape((bands * coarse_shape[0],) + coarse_shape[1:])
    norms = [
        merged(got_stats[:, level], own[level] * feats[level].shape[1], norm_gain[level], norm_shift[level])
        for level in range(3)
    ]

    def whole_norm(values, layer):
        return merged(
            local_stats(values)[None], values.shape[0] * values.shape[1], norm_gain[layer], norm_shift[layer]
        )

    def clamped(active, ring):
        count = active.shape[0]
        rows = jnp.arange(count)[:, None, None]
        active = jnp.where(first & (rows < ring), active[ring][None], active)
        return jnp.where(last & (rows >= count - ring), active[count - ring - 1][None], active)

    def doubled(active):
        return widen(heighten(active.astype(jnp.float32)))

    def zero_outside(rows_up, ring):
        count = rows_up.shape[0]
        rows = jnp.arange(count)[:, None, None]
        outside = (first & (rows < ring)) | (last & (rows >= count - ring))
        return jnp.where(outside, 0.0, rows_up).astype(jnp.bfloat16)

    active = clamped(act(fields[2], norms[2]), 2)
    field4 = conv_rows(zero_outside(doubled(active), 2), inner_weights[0])
    active = act(coarse, whole_norm(coarse, 3))
    framed = doubled(jnp.pad(active, ((1, 1), (0, 0), (0, 0)), mode="edge"))
    field5 = conv_rows(jnp.pad(framed.astype(jnp.bfloat16), ((1, 1), (0, 0), (0, 0))), inner_weights[1])
    active = jnp.pad(act(field5, whole_norm(field5, 5)), ((2, 2), (0, 0), (0, 0)), mode="edge")
    active = lax.dynamic_slice_in_dim(active, position * own[2], own[2] + 4, axis=0)
    field6 = conv_rows(zero_outside(doubled(active), 2), inner_weights[2])
    inner_stats = jnp.stack([local_stats(field4[1:-1]), local_stats(field6[1:-1])]).reshape(4, -1)
    got_stats = everyone(inner_stats, ROWS, bands).reshape(bands, 2, 2, head)
    pixels = own[1] * feats[1].shape[1]
    norm4 = merged(got_stats[:, 0], pixels, norm_gain[4], norm_shift[4])
    norm6 = merged(got_stats[:, 1], pixels, norm_gain[6], norm_shift[6])
    quarter = act(inner[0], norms[0])
    eighth_sum = (
        act(fields[1], norms[1]).astype(jnp.float32)
        + act(field4, norm4).astype(jnp.float32)
        + act(field6, norm6).astype(jnp.float32)
    )
    combined = (quarter.astype(jnp.float32) + doubled(clamped(eighth_sum, 1))).astype(jnp.bfloat16)
    scores = (
        jnp.einsum("rwc,ck->krw", combined, class_weight, preferred_element_type=jnp.float32)
        + class_bias[:, None, None]
    )
    log_total = jnp.log(jnp.sum(jnp.exp(scores), axis=0))
    label_map = labels[0]
    classes = jnp.arange(scores.shape[0], dtype=jnp.int32)[:, None, None]
    picked = jnp.sum(jnp.where(classes == label_map[None], scores, 0.0), axis=0)
    usable = label_map != 255
    local = jnp.stack(
        [jnp.sum(jnp.where(usable, log_total - picked, 0.0)), jnp.sum(usable.astype(jnp.float32))]
    )
    row = jnp.pad(local, (0, 126))[None]
    loss_total, valid_count = jnp.sum(everyone(row, EVERY, 8 * bands), axis=(0, 1))[:2]
    mean_loss = loss_total / jnp.maximum(valid_count, 1.0)
    return (scores.astype(jnp.bfloat16)[None], mean_loss)


def solution(mesh):
    split = Mesh(mesh.devices.reshape(4, 2, 4, 4), ("batch_0", "batch_1", "rows_0", "rows_1"))
    in_specs = (
        P(BATCH, ROWS, None, None),
        P(BATCH, ROWS, None, None),
        P(BATCH, ROWS, None, None),
        P(BATCH, ROWS, None, None),
        P(BATCH, ROWS, None),
        P(),
        P(),
        P(),
        P(),
        P(),
        P(),
    )
    out_specs = (P(BATCH, None, ROWS, None), P())
    return jax.shard_map(
        per_device, mesh=split, in_specs=in_specs, out_specs=out_specs, check_vma=False
    )
```

```python
import jax
import jax.numpy as jnp
import numpy as np
from jax import lax
from jax.experimental import pallas as pl
from jax.experimental.pallas import tpu as pltpu
from jax.sharding import Mesh
from jax.sharding import PartitionSpec as P

GROUPS = 32
GROUP = 4
HEAD = 128
ROWS = ("rows_0", "rows_1")
EVERY = ("batch_0", "batch_1", "rows_0", "rows_1")
BATCH = ("batch_0", "batch_1")
NORM_FLOOR = 0.05
DEPTHS = (1, 2, 3, 1)
STAT_ROWS = 48
SLOT = 32
F32, BF16 = jnp.float32, jnp.bfloat16
VMEM_LIMIT = 60 * 1024 * 1024


def doubling(cols):
    matrix = np.zeros((2 * cols, cols), np.float32)
    for k in range(cols):
        matrix[2 * k, k] += 0.75
        matrix[2 * k, max(k - 1, 0)] += 0.25
        matrix[2 * k + 1, k] += 0.75
        matrix[2 * k + 1, min(k + 1, cols - 1)] += 0.25
    return matrix


def everyone(pieces, axes):
    return lax.all_to_all(pieces, axes, 0, 0)


def matmul(a, b):
    return jnp.dot(a, b, preferred_element_type=F32)


def matmul_t(a, b):
    return lax.dot_general(a, b, (((1,), (1,)), ((), ())), preferred_element_type=F32)


def fill_pair(w_ref, out_ref, depth):
    zero = jnp.zeros((depth, HEAD), BF16)
    for j in range(4):
        for across in range(3):
            rows = slice(j * depth, (j + 1) * depth)
            at = across * 2 * HEAD
            out_ref[rows, at : at + HEAD] = w_ref[j, across] if j < 3 else zero
            out_ref[rows, at + HEAD : at + 2 * HEAD] = w_ref[j - 1, across] if j else zero


def fill_single(w_ref, out_ref, depth):
    for j in range(3):
        for across in range(3):
            out_ref[j * depth : (j + 1) * depth, across * HEAD : (across + 1) * HEAD] = w_ref[j, across]


def across_taps(z, width):
    pixels = z.shape[0]
    index = lax.broadcasted_iota(jnp.int32, (pixels, width), 0)
    left = jnp.where(index == 0, 0.0, pltpu.roll(z[:, :width], 1, 0))
    right = jnp.where(index == pixels - 1, 0.0, pltpu.roll(z[:, 2 * width :], pixels - 1, 0))
    return z[:, width : 2 * width] + left + right


def conv_pair(rows, w_ref):
    return across_taps(matmul(jnp.concatenate(rows, axis=1), w_ref[...]), 2 * HEAD)


def sums(y):
    total = jnp.sum(y, axis=0, keepdims=True)
    centred = y - total * (1.0 / y.shape[0])
    return total, jnp.sum(centred * centred, axis=0, keepdims=True)


def merge(parts, pixels):
    total = sum(p[0] for p in parts)
    mean = total * (1.0 / (pixels * len(parts)))
    square = sum(p[1] + pixels * jnp.square(p[0] * (1.0 / pixels) - mean) for p in parts)
    return total, square


def halves(pair):
    total, square = pair
    return [(total[:, :HEAD], square[:, :HEAD]), (total[:, HEAD:], square[:, HEAD:])]


def group_sum(v):
    lane = lax.broadcasted_iota(jnp.int32, v.shape, 1)
    v = v + jnp.where(lane % 2 == 0, pltpu.roll(v, HEAD - 1, 1), pltpu.roll(v, 1, 1))
    return v + jnp.where(lane % 4 < 2, pltpu.roll(v, HEAD - 2, 1), pltpu.roll(v, 2, 1))


def normed(y, mean, factor, shift):
    return jnp.maximum((y - mean) * factor + shift, 0.0).astype(BF16)


def split_rows(values):
    high = values.astype(BF16).astype(F32)
    rest = values - high
    middle = rest.astype(BF16).astype(F32)
    return [high, middle, rest - middle]


def edges_kernel(quarter, eighth, sixteenth, thirty, before, after, sems):
    copies, at = [], 0
    for level, feat in enumerate((quarter, eighth, sixteenth, thirty)):
        rows, cols, _ = feat.shape
        for i in range(DEPTHS[level]):
            spot = pl.ds(at + i * cols, cols)
            copies.append((feat.at[rows - DEPTHS[level] + i], before.at[spot]))
            copies.append((feat.at[i], after.at[spot]))
        at += DEPTHS[level] * cols
    started = [pltpu.make_async_copy(a, b, sems.at[i]) for i, (a, b) in enumerate(copies)]
    for copy in started:
        copy.start()
    for copy in started:
        copy.wait()


def inside_kernel(quarter, eighth, w0, w1, y0, y1, stats, wide0, wide1):
    fill_pair(w0, wide0, 2 * HEAD)
    fill_pair(w1, wide1, 2 * HEAD)
    stats[...] = jnp.zeros_like(stats)

    def work(x, wide, y, first):
        def step(p, carry):
            out = conv_pair([x[2 * p + j] for j in range(4)], wide)
            y[2 * p] = out[:, :HEAD]
            y[2 * p + 1] = out[:, HEAD:]
            total, square = sums(out)
            stats[first + p, 0:1] = total
            stats[first + p, 1:2] = square
            return carry

        lax.fori_loop(0, y.shape[0] // 2, step, 0)

    work(quarter, wide0, y0, 0)
    work(eighth, wide1, y1, y0.shape[0] // 2)


def outside_kernel(
    before, after, q_low, q_high, e_low, e_high, sixteenth, thirty, w0, w1, w2, w3, stats_in,
    y0, y1, y2, pieces, single0, wide1, wide2, wide3,
):
    depth = 2 * HEAD
    fill_single(w0, single0, depth)
    fill_pair(w1, wide1, depth)
    fill_pair(w2, wide2, depth)
    fill_pair(w3, wide3, depth)
    spots, at = [], 0
    cols = (q_low.shape[1], e_low.shape[1], sixteenth.shape[1], thirty.shape[1])
    for level in range(4):
        spots.append([slice(at + i * cols[level], at + (i + 1) * cols[level]) for i in range(DEPTHS[level])])
        at += DEPTHS[level] * cols[level]
    inside0 = 7
    quarter_parts, eighth_parts = [], []
    for p in range(inside0):
        quarter_parts += halves((stats_in[p, 0:1], stats_in[p, 1:2]))
    for p in range(inside0, inside0 + 3):
        eighth_parts += halves((stats_in[p, 0:1], stats_in[p, 1:2]))
    row_sets = (
        [before[spots[0][0]], q_low[0], q_low[1]],
        [q_high[0], q_high[1], after[spots[0][0]]],
    )
    for i, rows in enumerate(row_sets):
        out = across_taps(matmul(jnp.concatenate(rows, axis=1), single0[...]), HEAD)
        y0[i] = out
        quarter_parts.append(sums(out))
    row_sets = (
        [before[spots[1][0]], before[spots[1][1]], e_low[0], e_low[1]],
        [e_high[0], e_high[1], after[spots[1][0]], after[spots[1][1]]],
    )
    for i, rows in enumerate(row_sets):
        out = conv_pair(rows, wide1)
        y1[2 * i] = out[:, :HEAD]
        y1[2 * i + 1] = out[:, HEAD:]
        eighth_parts.append(halves(sums(out))[1 - i])
    rows = [before[s] for s in spots[2]]
    rows += [sixteenth[i] for i in range(sixteenth.shape[0])]
    rows += [after[s] for s in spots[2]]
    sixteenth_parts = []
    for p in range(y2.shape[0] // 2):
        out = conv_pair(rows[2 * p : 2 * p + 4], wide2)
        y2[2 * p] = out[:, :HEAD]
        y2[2 * p + 1] = out[:, HEAD:]
        if 0 < p < y2.shape[0] // 2 - 1:
            sixteenth_parts += halves(sums(out))
    out = conv_pair([before[spots[3][0]], thirty[0], thirty[1], after[spots[3][0]]], wide3)
    coarse = jnp.concatenate([out[:, :HEAD], out[:, HEAD:]], axis=0).astype(BF16)
    merged = [
        merge(quarter_parts, cols[0]), merge(eighth_parts, cols[1]), merge(sixteenth_parts, cols[2])
    ]
    pad = [jnp.zeros((5, HEAD), F32)]
    total = jnp.concatenate([m[0] for m in merged] + pad, axis=0)
    square = jnp.concatenate([m[1] for m in merged] + pad, axis=0)
    head = jnp.concatenate(split_rows(total) + split_rows(square), axis=0).astype(BF16)
    for i in range(pieces.shape[0]):
        pieces[i, :STAT_ROWS] = head
        pieces[i, STAT_ROWS:] = coarse


def between_kernel(
    place, got, y2, weights, gain, shift, up_small, up_big,
    y4, y6, params, pieces, fine, coarse, field5, stats5, wide0, wide1, wide2,
):
    members = got.shape[0]
    position = place[0]
    first, last = position == 0, position == members - 1
    for i, wide in enumerate((wide0, wide1, wide2)):
        fill_pair(weights.at[i], wide, HEAD)
    row = lax.broadcasted_iota(jnp.int32, (8, HEAD), 0)
    pixels = jnp.where(row == 0, 8192.0, jnp.where(row == 1, 2048.0, 512.0))

    def parts(i):
        block = got[i, :STAT_ROWS].astype(F32)
        return block[0:8] + block[8:16] + block[16:24], block[24:32] + block[32:40] + block[40:48]

    each = [parts(i) for i in range(members)]
    total = sum(p[0] for p in each)
    mean = group_sum(total) / (pixels * (members * GROUP))
    square = sum(p[1] + pixels * jnp.square(p[0] / pixels - mean) for p in each)
    var = group_sum(square) / (pixels * (members * GROUP))
    params[0] = mean
    params[1] = gain[...] * lax.rsqrt(var + NORM_FLOOR)
    params[2] = shift[...]

    def one(i, j):
        return params[i, j : j + 1]

    def local_norm(total, square, pixels, layer):
        total, square = (jnp.broadcast_to(v, (8, HEAD)) for v in (total, square))
        mean = group_sum(total) / (pixels * GROUP)
        square = square + pixels * jnp.square(total / pixels - mean)
        var = group_sum(square) / (pixels * GROUP)
        factor = gain[layer : layer + 1] * lax.rsqrt(var[0:1] + NORM_FLOOR)
        return mean[0:1], factor, shift[layer : layer + 1]

    def up_conv(acts, wide, out):
        count = len(acts)
        doubled = []
        for k in range(0, count, 2):
            both = matmul(up_big[...], jnp.concatenate([acts[k], acts[k + 1]], axis=1))
            doubled += [both[:, :HEAD], both[:, HEAD:]]
        lines = 2 * (count - 2)
        for k in range(1, count - 1):
            for half, other in ((0, k - 1), (1, k + 1)):
                line = 0.75 * doubled[k] + 0.25 * doubled[other]
                at = 2 * (k - 1) + half
                if at < 2:
                    line = jnp.where(first, 0.0, line)
                if at >= lines - 2:
                    line = jnp.where(last, 0.0, line)
                fine[at] = line.astype(BF16)
        own = []
        for p in range(lines // 2 - 1):
            y = conv_pair([fine[2 * p + j] for j in range(4)], wide)
            out[2 * p] = y[:, :HEAD]
            out[2 * p + 1] = y[:, HEAD:]
            two = halves(sums(y))
            own += two[1:] if p == 0 else two[:1] if p == lines // 2 - 2 else two
        return merge(own, y.shape[0])

    acts = [normed(y2[i], one(0, 2), one(1, 2), one(2, 2)) for i in range(y2.shape[0])]
    count = len(acts)
    acts[1] = jnp.where(first, acts[2], acts[1])
    acts[count - 2] = jnp.where(last, acts[count - 3], acts[count - 2])
    merged4 = up_conv(acts, wide0, y4)
    lines, cols = coarse.shape[0] - 2, coarse.shape[1]
    small = cols // 2
    total3 = jnp.zeros((1, HEAD), F32)
    for i in range(members):
        total3 = total3 + jnp.sum(got[i, STAT_ROWS:].astype(F32), axis=0, keepdims=True)
    count3 = members * 2 * small
    middle3 = total3 * (1.0 / count3)
    square3 = jnp.zeros((1, HEAD), F32)
    for i in range(members):
        square3 = square3 + jnp.sum(
            jnp.square(got[i, STAT_ROWS:].astype(F32) - middle3), axis=0, keepdims=True
        )
    norm3 = local_norm(total3, square3, count3, 3)
    doubled = []
    for i in range(members):
        a = normed(got[i, STAT_ROWS:].astype(F32), *norm3)
        both = matmul(up_small[...], jnp.concatenate([a[:small], a[small:]], axis=1))
        doubled += [both[:, :HEAD], both[:, HEAD:]]
    coarse[0] = jnp.zeros((cols, HEAD), BF16)
    coarse[lines + 1] = jnp.zeros((cols, HEAD), BF16)
    for k in range(len(doubled)):
        for half, other in ((0, max(k - 1, 0)), (1, min(k + 1, len(doubled) - 1))):
            coarse[1 + 2 * k + half] = (0.75 * doubled[k] + 0.25 * doubled[other]).astype(BF16)

    def step(p, carry):
        y = conv_pair([coarse[2 * p + j] for j in range(4)], wide1)
        field5[2 * p] = y[:, :HEAD]
        field5[2 * p + 1] = y[:, HEAD:]
        total, square = sums(y)
        stats5[p, 0:1] = total
        stats5[p, 1:2] = square
        return carry

    lax.fori_loop(0, lines // 2, step, 0)
    parts5 = []
    for p in range(lines // 2):
        parts5 += halves((stats5[p, 0:1], stats5[p, 1:2]))
    total5, square5 = merge(parts5, cols)
    norm5 = local_norm(total5, square5, lines * cols, 5)
    band = lines // members
    acts = []
    for i in range(band + 4):
        at = jnp.clip(position * band + (i - 2), 0, lines - 1)
        acts.append(normed(field5[at], *norm5))
    merged6 = up_conv(acts, wide2, y6)
    block = jnp.concatenate(
        [merged4[0], merged6[0], jnp.zeros((6, HEAD), F32), merged4[1], merged6[1], jnp.zeros((6, HEAD), F32)],
        axis=0,
    )
    for i in range(members):
        pieces[i] = block


def final_kernel(
    place, bias, got, params, gain, shift, y0, y0_edge, y1, y1_edge, y4, y6, labels, class_t, class_t3, up_cols,
    logits, pieces, lines, scores,
):
    members = got.shape[0]
    first, last = place[0] == 0, place[0] == members - 1
    pixels = 2048.0
    total = sum(got[i, 0:8] for i in range(members))
    mean = group_sum(total) / (pixels * members * GROUP)
    square = sum(got[i, 8:16] + pixels * jnp.square(got[i, 0:8] / pixels - mean) for i in range(members))
    var = group_sum(square) / (pixels * members * GROUP)
    scale = lax.rsqrt(var + NORM_FLOOR)
    norm4 = (mean[0:1], gain[4:5] * scale[0:1], shift[4:5])
    norm6 = (mean[1:2], gain[6:7] * scale[1:2], shift[6:7])
    norm0 = tuple(params[i, 0:1] for i in range(3))
    norm1 = tuple(params[i, 1:2] for i in range(3))
    count = y4.shape[0]
    for i in range(count):
        field1 = y1_edge[i] if i < 2 else y1_edge[i - count + 4] if i >= count - 2 else y1[i - 2]
        acts = jnp.concatenate(
            [normed(field1, *norm1), normed(y4[i], *norm4), normed(y6[i], *norm6)], axis=1
        )
        lines[i] = matmul_t(class_t3[...], acts)
    lines[0] = jnp.where(first, lines[1], lines[0])
    lines[count - 1] = jnp.where(last, lines[count - 2], lines[count - 1])
    doubled = []
    for i in range(count):
        value = lines[i]
        high = value.astype(BF16)
        low = (value - high.astype(F32)).astype(BF16)
        doubled.append(matmul(jnp.concatenate([high, low], axis=0), up_cols[...]))
    doubled = [d[:SLOT] + d[SLOT:] for d in doubled]
    rows = labels.shape[0]
    for r in range(rows):
        field0 = y0_edge[0] if r == 0 else y0_edge[1] if r == rows - 1 else y0[r - 1]
        k = r // 2 + 1
        other = k - 1 if r % 2 == 0 else k + 1
        value = matmul_t(class_t[...], normed(field0, *norm0))
        value = value + (0.75 * doubled[k] + 0.25 * doubled[other])
        for i in range(scores.shape[0]):
            scores[i, r * SLOT : (r + 1) * SLOT] = value[:, i * HEAD : (i + 1) * HEAD]
    label_map = labels[...]
    exps = jnp.zeros(label_map.shape, F32)
    picked = jnp.zeros(label_map.shape, F32)
    for c in range(logits.shape[0]):
        tiles = [scores.at[i][pl.ds(c, rows, stride=SLOT), :] for i in range(scores.shape[0])]
        score = jnp.concatenate(tiles, axis=1) + bias[c]
        logits[c] = score.astype(BF16)
        exps = exps + jnp.exp(score)
        picked = picked + jnp.where(label_map == c, score, 0.0)
    usable = label_map != 255
    terms = jnp.where(usable, jnp.log(exps) - picked, 0.0)
    counts = jnp.where(usable, 1.0, 0.0)
    out = []
    for v in (terms, counts):
        v = jnp.sum(v, axis=0, keepdims=True)
        out.append(sum(v[:, i * HEAD : (i + 1) * HEAD] for i in range(v.shape[1] // HEAD)))
    block = jnp.concatenate(out, axis=0)
    for i in range(pieces.shape[0]):
        pieces[i] = block


def params_of(**kw):
    return pltpu.CompilerParams(vmem_limit_bytes=VMEM_LIMIT, **kw)


def shaped(shape, dtype):
    return jax.ShapeDtypeStruct(shape, dtype)


VM = pl.BlockSpec(memory_space=pltpu.VMEM)
SM = pl.BlockSpec(memory_space=pltpu.SMEM)
ANY = pl.BlockSpec(memory_space=pl.ANY)


def block(shape, index):
    return pl.BlockSpec(shape, lambda i: index)


def per_device(
    feat_quarter,
    feat_eighth,
    feat_sixteenth,
    feat_thirty,
    labels,
    first_weights,
    inner_weights,
    norm_gain,
    norm_shift,
    class_weight,
    class_bias,
):
    position = lax.axis_index(ROWS)
    bands = lax.axis_size(ROWS)
    devices = bands * lax.axis_size(BATCH)
    place = position.astype(jnp.int32).reshape(1)
    up_pairs = [(i, i + 1) for i in range(bands - 1)]
    down_pairs = [(j, i) for i, j in up_pairs]
    feats = [feat_quarter[0], feat_eighth[0], feat_sixteenth[0], feat_thirty[0]]
    depth = feats[0].shape[2]
    halo = sum(d * f.shape[1] for d, f in zip(DEPTHS, feats))
    before, after = pl.pallas_call(
        edges_kernel,
        out_shape=[shaped((halo, depth), BF16)] * 2,
        in_specs=[ANY] * 4,
        out_specs=[ANY] * 2,
        scratch_shapes=[pltpu.SemaphoreType.DMA((2 * sum(DEPTHS),))],
        name="edges",
    )(*feats)
    before = lax.ppermute(before, ROWS, up_pairs)
    after = lax.ppermute(after, ROWS, down_pairs)
    q_rows, q_cols, _ = feats[0].shape
    e_rows, e_cols, _ = feats[1].shape
    s_rows, s_cols, _ = feats[2].shape
    t_rows, t_cols, _ = feats[3].shape
    wide = pltpu.VMEM((4 * depth, 6 * HEAD), BF16)
    y0, y1, stats = pl.pallas_call(
        inside_kernel,
        out_shape=[
            shaped((q_rows - 2, q_cols, HEAD), F32),
            shaped((e_rows - 2, e_cols, HEAD), F32),
            shaped(((q_rows + e_rows) // 2 - 2, 8, 2 * HEAD), F32),
        ],
        in_specs=[VM] * 4,
        out_specs=[VM] * 3,
        scratch_shapes=[wide, wide],
        compiler_params=params_of(),
        name="inside",
    )(feats[0], feats[1], first_weights[0], first_weights[1])
    whole = lambda a: block(a.shape, (0,) * a.ndim)
    args = [before, after, feats[0], feats[0], feats[1], feats[1], feats[2], feats[3]]
    specs = [
        whole(before), whole(after),
        block((2, q_cols, depth), (0, 0, 0)), block((2, q_cols, depth), (q_rows // 2 - 1, 0, 0)),
        block((2, e_cols, depth), (0, 0, 0)), block((2, e_cols, depth), (e_rows // 2 - 1, 0, 0)),
        whole(feats[2]), whole(feats[3]),
    ]
    for level in range(4):
        args.append(first_weights)
        specs.append(block((None,) + first_weights.shape[1:], (level, 0, 0, 0, 0)))
    args.append(stats)
    specs.append(whole(stats))
    piece = STAT_ROWS + t_rows * t_cols
    out_shape = [
        shaped((2, q_cols, HEAD), F32),
        shaped((4, e_cols, HEAD), F32),
        shaped((s_rows + 4, s_cols, HEAD), F32),
        shaped((bands, piece, HEAD), BF16),
    ]
    y0_edge, y1_edge, y2, pieces = pl.pallas_call(
        outside_kernel,
        grid=(1,),
        out_shape=out_shape,
        in_specs=specs,
        out_specs=[whole(s) for s in out_shape],
        scratch_shapes=[pltpu.VMEM((3 * depth, 3 * HEAD), BF16), wide, wide, wide],
        compiler_params=params_of(),
        name="outside",
    )(*args)
    got = everyone(pieces, ROWS)
    up_small = jnp.asarray(doubling(t_cols), BF16)
    up_big = jnp.asarray(doubling(s_cols), BF16)
    up_cols = jnp.asarray(doubling(e_cols).T, BF16)
    pad = ((0, 1), (0, 0))
    gain8, shift8 = jnp.pad(norm_gain, pad), jnp.pad(norm_shift, pad)
    narrow = pltpu.VMEM((4 * HEAD, 6 * HEAD), BF16)
    y4, y6, params, pieces = pl.pallas_call(
        between_kernel,
        out_shape=[
            shaped((e_rows + 2, e_cols, HEAD), F32),
            shaped((e_rows + 2, e_cols, HEAD), F32),
            shaped((3, 8, HEAD), F32),
            shaped((bands, 16, HEAD), F32),
        ],
        in_specs=[SM] + [VM] * 7,
        out_specs=[VM] * 4,
        scratch_shapes=[
            pltpu.VMEM((e_rows + 4, e_cols, HEAD), BF16),
            pltpu.VMEM((2 * t_rows * bands + 2, 2 * t_cols, HEAD), BF16),
            pltpu.VMEM((2 * t_rows * bands, 2 * t_cols, HEAD), F32),
            pltpu.VMEM((t_rows * bands, 8, 2 * HEAD), F32),
            narrow, narrow, narrow,
        ],
        compiler_params=params_of(),
        name="between",
    )(place, got, y2, inner_weights, gain8, shift8, up_small, up_big)
    got = everyone(pieces, ROWS)
    classes = class_weight.shape[1]
    class_t = jnp.pad(class_weight.T, ((0, SLOT - classes), (0, 0)))
    class_t3 = jnp.concatenate([class_t] * 3, axis=1)
    logits, pieces = pl.pallas_call(
        final_kernel,
        out_shape=[shaped((classes, q_rows, q_cols), BF16), shaped((devices, 2, HEAD), F32)],
        in_specs=[SM, SM] + [VM] * 14,
        out_specs=[VM] * 2,
        scratch_shapes=[
            pltpu.VMEM((e_rows + 2, SLOT, e_cols), F32),
            pltpu.VMEM((q_cols // HEAD, q_rows * SLOT, HEAD), F32),
        ],
        compiler_params=params_of(),
        name="final",
    )(
        place, class_bias, got, params, gain8, shift8, y0, y0_edge, y1, y1_edge, y4, y6, labels[0],
        class_t, class_t3, up_cols,
    )
    loss_total, valid_count = jnp.sum(everyone(pieces, EVERY), axis=(0, 2))
    mean_loss = loss_total / jnp.maximum(valid_count, 1.0)
    return (logits[None], mean_loss)


def solution(mesh):
    split = Mesh(mesh.devices.reshape(4, 2, 4, 4), ("batch_0", "batch_1", "rows_0", "rows_1"))
    in_specs = (
        P(BATCH, ROWS, None, None),
        P(BATCH, ROWS, None, None),
        P(BATCH, ROWS, None, None),
        P(BATCH, ROWS, None, None),
        P(BATCH, ROWS, None),
        P(),
        P(),
        P(),
        P(),
        P(),
        P(),
    )
    out_specs = (P(BATCH, None, ROWS, None), P())
    return jax.shard_map(
        per_device, mesh=split, in_specs=in_specs, out_specs=out_specs, check_vma=False
    )
```

```python
import jax
import jax.numpy as jnp
import numpy as np
from jax import lax
from jax.experimental import pallas as pl
from jax.experimental.pallas import tpu as pltpu
from jax.sharding import Mesh
from jax.sharding import PartitionSpec as P

GROUP = 4
HEAD = 128
ROWS = ("rows_0", "rows_1")
EVERY = ("batch_0", "batch_1", "rows_0", "rows_1")
BATCH = ("batch_0", "batch_1")
NORM_FLOOR = 0.05
SMALL = (3, 1)
BIG = (1, 2)
STAT_ROWS = 32
EARLY = 3
SLOT = 32
F32, BF16 = jnp.float32, jnp.bfloat16
VMEM_LIMIT = 60 * 1024 * 1024


def doubling(cols):
    matrix = np.zeros((2 * cols, cols), np.float32)
    for k in range(cols):
        matrix[2 * k, k] += 0.75
        matrix[2 * k, max(k - 1, 0)] += 0.25
        matrix[2 * k + 1, k] += 0.75
        matrix[2 * k + 1, min(k + 1, cols - 1)] += 0.25
    return matrix


def everyone(pieces, axes):
    return lax.all_to_all(pieces, axes, 0, 0)


def matmul(a, b):
    return jnp.dot(a, b, preferred_element_type=F32)


def matmul_t(a, b):
    return lax.dot_general(a, b, (((1,), (1,)), ((), ())), preferred_element_type=F32)


def fill_pair(w_ref, out_ref, depth):
    zero = jnp.zeros((depth, HEAD), BF16)
    for j in range(4):
        for across in range(3):
            rows = slice(j * depth, (j + 1) * depth)
            at = across * 2 * HEAD
            out_ref[rows, at : at + HEAD] = w_ref[j, across] if j < 3 else zero
            out_ref[rows, at + HEAD : at + 2 * HEAD] = w_ref[j - 1, across] if j else zero


def across_taps(z, width, cols):
    pixels = z.shape[0]
    index = lax.broadcasted_iota(jnp.int32, (pixels, width), 0) % cols
    left = jnp.where(index == 0, 0.0, pltpu.roll(z[:, :width], 1, 0))
    right = jnp.where(index == cols - 1, 0.0, pltpu.roll(z[:, 2 * width :], pixels - 1, 0))
    return z[:, width : 2 * width] + left + right


def conv_pair(rows, w_ref):
    return across_taps(matmul(jnp.concatenate(rows, axis=1), w_ref[...]), 2 * HEAD, rows[0].shape[0])


def sums(y):
    total = jnp.sum(y, axis=0, keepdims=True)
    centred = y - total * (1.0 / y.shape[0])
    return total, jnp.sum(centred * centred, axis=0, keepdims=True)


def merge(parts, pixels):
    total = sum(p[0] for p in parts)
    mean = total * (1.0 / (pixels * len(parts)))
    square = sum(p[1] + pixels * jnp.square(p[0] * (1.0 / pixels) - mean) for p in parts)
    return total, square


def halves(pair):
    total, square = pair
    return [(total[:, :HEAD], square[:, :HEAD]), (total[:, HEAD:], square[:, HEAD:])]


def group_sum(v):
    lane = lax.broadcasted_iota(jnp.int32, v.shape, 1)
    v = v + jnp.where(lane % 2 == 0, pltpu.roll(v, HEAD - 1, 1), pltpu.roll(v, 1, 1))
    return v + jnp.where(lane % 4 < 2, pltpu.roll(v, HEAD - 2, 1), pltpu.roll(v, 2, 1))


def normed(y, mean, factor, shift):
    return jnp.maximum((y - mean) * factor + shift, 0.0).astype(BF16)


def split_rows(values):
    high = values.astype(BF16).astype(F32)
    rest = values - high
    middle = rest.astype(BF16).astype(F32)
    return [high, middle, rest - middle]


def edges_kernel(quarter, eighth, sixteenth, thirty, small_before, small_after, big_before, big_after, sems):
    copies = []
    groups = (
        (SMALL, (sixteenth, thirty), small_before, small_after),
        (BIG, (quarter, eighth), big_before, big_after),
    )
    for depths, feats, before, after in groups:
        at = 0
        for depth, feat in zip(depths, feats):
            rows, cols, _ = feat.shape
            for i in range(depth):
                spot = pl.ds(at, cols)
                copies.append((feat.at[rows - depth + i], before.at[spot]))
                copies.append((feat.at[i], after.at[spot]))
                at += cols
    started = [pltpu.make_async_copy(a, b, sems.at[i]) for i, (a, b) in enumerate(copies)]
    for copy in started:
        copy.start()
    for copy in started:
        copy.wait()


def store_pair(out, y, stats, step):
    y[0] = out[:, :HEAD]
    y[1] = out[:, HEAD:]
    total, square = sums(out)
    stats[step, 0:1] = total
    stats[step, 1:2] = square


def quarter_early_kernel(low, middle, high, w, y, stats, wide):
    step = pl.program_id(0)

    @pl.when(step == 0)
    def _():
        fill_pair(w, wide, 2 * HEAD)

    store_pair(conv_pair([low[0], middle[0], middle[1], high[0]], wide), y, stats, step)


def quarter_late_kernel(low, middle, high, before, after, w, _, __, y, stats, wide):
    step = pl.program_id(0)

    @pl.when(step == 0)
    def _():
        fill_pair(w, wide, 2 * HEAD)

    above = jnp.where(step == 0, before[...], low[0])
    below = jnp.where(step == pl.num_programs(0) - 1, after[...], high[0])
    store_pair(conv_pair([above, middle[0], middle[1], below], wide), y, stats, step)


def eighth_kernel(low, high, before, after, w, _, y, stats, wide):
    step = pl.program_id(0)
    cols = low.shape[1]

    @pl.when(step == 0)
    def _():
        fill_pair(w, wide, 2 * HEAD)

    at_first, at_last = step == 0, step == pl.num_programs(0) - 1
    rows = [jnp.where(at_first, before[i * cols : (i + 1) * cols], low[i]) for i in range(2)]
    rows += [jnp.where(at_last, after[i * cols : (i + 1) * cols], high[i]) for i in range(2)]
    store_pair(conv_pair(rows, wide), y, stats, step)


def coarse_kernel(before, after, sixteenth, thirty, w2, w3, _, y2, pieces, wide2, wide3):
    depth = 2 * HEAD
    fill_pair(w2, wide2, depth)
    fill_pair(w3, wide3, depth)
    own, cols, _ = sixteenth.shape
    ring = SMALL[0]
    rows = [before[i * cols : (i + 1) * cols] for i in range(ring)]
    rows += [sixteenth[i] for i in range(own)]
    rows += [after[i * cols : (i + 1) * cols] for i in range(ring)]
    parts = []
    for p in range(y2.shape[0] // 2):
        out = conv_pair(rows[2 * p : 2 * p + 4], wide2)
        y2[2 * p] = out[:, :HEAD]
        y2[2 * p + 1] = out[:, HEAD:]
        if 0 < p < y2.shape[0] // 2 - 1:
            parts += halves(sums(out))
    at = ring * cols
    out = conv_pair([before[at:], thirty[0], thirty[1], after[at:]], wide3)
    coarse = jnp.concatenate([out[:, :HEAD], out[:, HEAD:]], axis=0).astype(BF16)
    total, square = merge(parts, cols)
    values = jnp.concatenate([total, square, jnp.zeros((6, HEAD), F32)], axis=0)
    head = jnp.concatenate(split_rows(values) + [jnp.zeros((8, HEAD), F32)], axis=0).astype(BF16)
    for i in range(pieces.shape[0]):
        pieces[i, :STAT_ROWS] = head
        pieces[i, STAT_ROWS:] = coarse


def between_kernel(
    place, got, y2, weights, gain, shift, up_small, up_big, stats_early, stats_late, stats_eighth,
    y4, y6, pieces, fine, coarse, field5, stats5, wide0, wide1, wide2,
):
    members = got.shape[0]
    position = place[0]
    first, last = position == 0, position == members - 1
    for i, wide in enumerate((wide0, wide1, wide2)):
        fill_pair(weights.at[i], wide, HEAD)

    def merged_norm(each, pixels, layer):
        count = pixels * len(each) * GROUP
        mean = group_sum(jnp.broadcast_to(sum(p[0] for p in each), (8, HEAD)))[0:1] * (1.0 / count)
        square = sum(p[1] + pixels * jnp.square(p[0] * (1.0 / pixels) - mean) for p in each)
        var = group_sum(jnp.broadcast_to(square, (8, HEAD)))[0:1] * (1.0 / count)
        return mean, gain[layer : layer + 1] * lax.rsqrt(var + NORM_FLOOR), shift[layer : layer + 1]

    def up_conv(acts, wide, out):
        count = len(acts)
        doubled = []
        for k in range(0, count, 2):
            both = matmul(up_big[...], jnp.concatenate([acts[k], acts[k + 1]], axis=1))
            doubled += [both[:, :HEAD], both[:, HEAD:]]
        lines = 2 * (count - 2)
        for k in range(1, count - 1):
            for half, other in ((0, k - 1), (1, k + 1)):
                line = 0.75 * doubled[k] + 0.25 * doubled[other]
                at = 2 * (k - 1) + half
                if at < 2:
                    line = jnp.where(first, 0.0, line)
                if at >= lines - 2:
                    line = jnp.where(last, 0.0, line)
                fine[at] = line.astype(BF16)
        own = []
        for p in range(lines // 2 - 1):
            y = conv_pair([fine[2 * p + j] for j in range(4)], wide)
            out[2 * p] = y[:, :HEAD]
            out[2 * p + 1] = y[:, HEAD:]
            two = halves(sums(y))
            own += two[1:] if p == 0 else two[:1] if p == lines // 2 - 2 else two
        return merge(own, y.shape[0])

    lines, cols = coarse.shape[0] - 2, coarse.shape[1]
    small = cols // 2
    each3 = [sums(got[i, STAT_ROWS:].astype(F32)) for i in range(members)]
    norm3 = merged_norm(each3, 2 * small, 3)
    doubled = []
    for i in range(members):
        a = normed(got[i, STAT_ROWS:].astype(F32), *norm3)
        both = matmul(up_small[...], jnp.concatenate([a[:small], a[small:]], axis=1))
        doubled += [both[:, :HEAD], both[:, HEAD:]]
    coarse[0] = jnp.zeros((cols, HEAD), BF16)
    coarse[lines + 1] = jnp.zeros((cols, HEAD), BF16)
    for k in range(len(doubled)):
        for half, other in ((0, max(k - 1, 0)), (1, min(k + 1, len(doubled) - 1))):
            coarse[1 + 2 * k + half] = (0.75 * doubled[k] + 0.25 * doubled[other]).astype(BF16)
    fold = 4

    def step(q, carry):
        base = q * (2 * fold)
        lhs = jnp.concatenate(
            [
                jnp.concatenate([coarse[base + 2 * i + j] for j in range(4)], axis=1)
                for i in range(fold)
            ],
            axis=0,
        )
        y = across_taps(matmul(lhs, wide1[...]), 2 * HEAD, cols)
        for i in range(fold):
            field5[base + 2 * i] = y[i * cols : (i + 1) * cols, :HEAD]
            field5[base + 2 * i + 1] = y[i * cols : (i + 1) * cols, HEAD:]
        total, square = sums(y)
        stats5[q, 0:1] = total
        stats5[q, 1:2] = square
        return carry

    lax.fori_loop(0, lines // (2 * fold), step, 0, unroll=2)
    blocks = [got[i, :STAT_ROWS].astype(F32) for i in range(members)]
    blocks = [b[0:8] + b[8:16] + b[16:24] for b in blocks]
    norm2 = merged_norm([(b[0:1], b[1:2]) for b in blocks], y2.shape[1] * (y2.shape[0] - 4), 2)
    acts = [normed(y2[i], *norm2) for i in range(y2.shape[0])]
    count = len(acts)
    acts[1] = jnp.where(first, acts[2], acts[1])
    acts[count - 2] = jnp.where(last, acts[count - 3], acts[count - 2])
    merged4 = up_conv(acts, wide0, y4)
    parts5 = []
    for q in range(lines // (2 * fold)):
        parts5 += halves((stats5[q, 0:1], stats5[q, 1:2]))
    norm5 = merged_norm(parts5, cols * fold, 5)
    band = lines // members
    acts = []
    for i in range(band + 4):
        at = jnp.clip(position * band + (i - 2), 0, lines - 1)
        acts.append(normed(field5[at], *norm5))
    merged6 = up_conv(acts, wide2, y6)
    parts0, parts1 = [], []
    for stats in (stats_early, stats_late):
        for p in range(stats.shape[0]):
            parts0 += halves((stats[p, 0:1], stats[p, 1:2]))
    for p in range(stats_eighth.shape[0]):
        two = halves((stats_eighth[p, 0:1], stats_eighth[p, 1:2]))
        parts1 += two[1:] if p == 0 else two[:1] if p == stats_eighth.shape[0] - 1 else two
    eighth_cols = y4.shape[1]
    merged = [merge(parts0, 2 * eighth_cols), merge(parts1, eighth_cols), merged4, merged6]
    pad = [jnp.zeros((4, HEAD), F32)]
    block = jnp.concatenate([m[0] for m in merged] + pad + [m[1] for m in merged] + pad, axis=0)
    for i in range(members):
        pieces[i] = block


def final_kernel(
    place, bias, got, gain, shift, y0, y1, y4, y6, labels, class_t, class_t3, up_cols,
    logits, pieces, lines, doubled, scores, norms,
):
    members = got.shape[0]
    step = pl.program_id(0)
    count = y4.shape[0]

    @pl.when(step == 0)
    def _():
        first, last = place[0] == 0, place[0] == members - 1
        row = lax.broadcasted_iota(jnp.int32, (8, HEAD), 0)
        own = float((count - 2) * y4.shape[1])
        pixels = jnp.where(row == 0, 4.0 * own, own)
        total = sum(got[i, 0:8] for i in range(members))
        mean = group_sum(total) / (pixels * (members * GROUP))
        square = sum(got[i, 8:16] + pixels * jnp.square(got[i, 0:8] / pixels - mean) for i in range(members))
        scale = lax.rsqrt(group_sum(square) / (pixels * (members * GROUP)) + NORM_FLOOR)
        layers = (0, 1, 4, 6)
        norm = [
            (mean[j : j + 1], gain[layer : layer + 1] * scale[j : j + 1], shift[layer : layer + 1])
            for j, layer in enumerate(layers)
        ]
        for i in range(3):
            norms[i : i + 1] = norm[0][i]
        for i in range(count):
            acts = [normed(y[i], *norm[1 + j]) for j, y in enumerate((y1, y4, y6))]
            lines[i] = matmul_t(class_t3[...], jnp.concatenate(acts, axis=1))
        lines[0] = jnp.where(first, lines[1], lines[0])
        lines[count - 1] = jnp.where(last, lines[count - 2], lines[count - 1])
        for i in range(count):
            value = lines[i]
            high = value.astype(BF16)
            low = (value - high.astype(F32)).astype(BF16)
            both = matmul(jnp.concatenate([high, low], axis=0), up_cols[...])
            doubled[i] = both[:SLOT] + both[SLOT:]

    norm0 = tuple(norms[i : i + 1] for i in range(3))
    centre = 0.75 * doubled[step + 1]
    for half in range(2):
        value = matmul_t(class_t[...], normed(y0[half], *norm0))
        value = value + (centre + 0.25 * doubled[step + 2 * half])
        at = pl.multiple_of((2 * step + half) * SLOT, SLOT)
        for i in range(scores.shape[0]):
            scores[i, pl.ds(at, SLOT)] = value[:, i * HEAD : (i + 1) * HEAD]

    @pl.when(step == pl.num_programs(0) - 1)
    def _():
        label_map = labels[...]
        rows = label_map.shape[0]
        exps = jnp.zeros(label_map.shape, F32)
        picked = jnp.zeros(label_map.shape, F32)
        for c in range(logits.shape[0]):
            tiles = [scores.at[i][pl.ds(c, rows, stride=SLOT), :] for i in range(scores.shape[0])]
            score = jnp.concatenate(tiles, axis=1) + bias[c]
            logits[c] = score.astype(BF16)
            exps = exps + jnp.exp(score)
            picked = picked + jnp.where(label_map == c, score, 0.0)
        usable = label_map != 255
        terms = jnp.where(usable, jnp.log(exps) - picked, 0.0)
        counts = jnp.where(usable, 1.0, 0.0)
        out = []
        for v in (terms, counts):
            v = jnp.sum(v, axis=0, keepdims=True)
            out.append(sum(v[:, i * HEAD : (i + 1) * HEAD] for i in range(v.shape[1] // HEAD)))
        both = jnp.concatenate(out, axis=0)
        for i in range(pieces.shape[0]):
            pieces[i] = both


def params_of(**kw):
    return pltpu.CompilerParams(vmem_limit_bytes=VMEM_LIMIT, **kw)


def shaped(shape, dtype):
    return jax.ShapeDtypeStruct(shape, dtype)


VM = pl.BlockSpec(memory_space=pltpu.VMEM)
SM = pl.BlockSpec(memory_space=pltpu.SMEM)
ANY = pl.BlockSpec(memory_space=pl.ANY)


def device_step(
    feat_quarter,
    feat_eighth,
    feat_sixteenth,
    feat_thirty,
    labels,
    first_weights,
    inner_weights,
    norm_gain,
    norm_shift,
    class_weight,
    class_bias,
):
    position = lax.axis_index(ROWS)
    bands = lax.axis_size(ROWS)
    devices = bands * lax.axis_size(BATCH)
    place = position.astype(jnp.int32).reshape(1)
    up_pairs = [(i, i + 1) for i in range(bands - 1)]
    down_pairs = [(j, i) for i, j in up_pairs]
    feats = [feat_quarter[0], feat_eighth[0], feat_sixteenth[0], feat_thirty[0]]
    quarter, eighth, sixteenth, thirty = feats
    q_rows, q_cols, depth = quarter.shape
    e_rows, e_cols, _ = eighth.shape
    s_rows, s_cols, _ = sixteenth.shape
    t_rows, t_cols, _ = thirty.shape
    small = shaped((SMALL[0] * s_cols + SMALL[1] * t_cols, depth), BF16)
    big = shaped((BIG[0] * q_cols + BIG[1] * e_cols, depth), BF16)
    small_before, small_after, big_before, big_after = pl.pallas_call(
        edges_kernel,
        out_shape=[small, small, big, big],
        in_specs=[ANY] * 4,
        out_specs=[VM] * 4,
        scratch_shapes=[pltpu.SemaphoreType.DMA((2 * (sum(SMALL) + sum(BIG)),))],
        compiler_params=params_of(),
        name="edges",
    )(*feats)
    small_before = lax.ppermute(small_before, ROWS, up_pairs)
    small_after = lax.ppermute(small_after, ROWS, down_pairs)
    big_before = lax.ppermute(big_before, ROWS, up_pairs)
    big_after = lax.ppermute(big_after, ROWS, down_pairs)

    def fixed(a, *index):
        index = index or (0,) * len(a.shape)
        return pl.BlockSpec(a.shape, lambda i: index)

    def weight(level):
        return pl.BlockSpec((None,) + first_weights.shape[1:], lambda i: (level, 0, 0, 0, 0))

    wide = pltpu.VMEM((4 * depth, 6 * HEAD), BF16)
    pairs = q_rows // 2
    line = (1, q_cols, depth)

    def quarter_specs(pair):
        return [
            pl.BlockSpec(line, lambda i: (jnp.maximum(2 * pair(i) - 1, 0), 0, 0)),
            pl.BlockSpec((2, q_cols, depth), lambda i: (pair(i), 0, 0)),
            pl.BlockSpec(line, lambda i: (jnp.minimum(2 * pair(i) + 2, q_rows - 1), 0, 0)),
        ]

    early = lambda i: i + 1
    late = lambda i: jnp.where(i == 0, 0, i + EARLY)
    field = shaped((q_rows, q_cols, HEAD), F32)
    stats_shape = lambda n: shaped((n, 8, 2 * HEAD), F32)
    early_call = pl.pallas_call(
        quarter_early_kernel,
        grid=(EARLY,),
        out_shape=[field, stats_shape(EARLY)],
        in_specs=quarter_specs(early) + [weight(0)],
        out_specs=[
            pl.BlockSpec((2, q_cols, HEAD), lambda i: (early(i), 0, 0)), fixed(stats_shape(EARLY))
        ],
        scratch_shapes=[wide],
        compiler_params=params_of(),
        name="quarter_early",
    )
    y0, stats_early = early_call(quarter, quarter, quarter, first_weights)
    piece = shaped((bands, STAT_ROWS + t_rows * t_cols, HEAD), BF16)
    y2_shape = shaped((s_rows + 4, s_cols, HEAD), F32)
    y2, pieces = pl.pallas_call(
        coarse_kernel,
        grid=(1,),
        out_shape=[y2_shape, piece],
        in_specs=[fixed(small), fixed(small), fixed(sixteenth), fixed(thirty), weight(2), weight(3), ANY],
        out_specs=[fixed(y2_shape), fixed(piece)],
        scratch_shapes=[wide, wide],
        compiler_params=params_of(),
        name="coarse",
    )(small_before, small_after, sixteenth, thirty, first_weights, first_weights, stats_early)
    got = everyone(pieces, ROWS)
    y0, stats_late = pl.pallas_call(
        quarter_late_kernel,
        grid=(pairs - EARLY,),
        out_shape=[field, stats_shape(pairs - EARLY)],
        in_specs=quarter_specs(late)
        + [pl.BlockSpec((q_cols, depth), lambda i: (0, 0))] * 2
        + [weight(0), ANY, ANY],
        out_specs=[
            pl.BlockSpec((2, q_cols, HEAD), lambda i: (late(i), 0, 0)), fixed(stats_shape(pairs - EARLY))
        ],
        input_output_aliases={6: 0},
        scratch_shapes=[wide],
        compiler_params=params_of(),
        name="quarter_late",
    )(quarter, quarter, quarter, big_before, big_after, first_weights, y0, y2)
    steps = e_rows // 2 + 1
    halo = pl.BlockSpec((BIG[1] * e_cols, depth), lambda i: (BIG[0] * q_cols // (BIG[1] * e_cols), 0))
    two = (2, e_cols, depth)
    y1, stats_eighth = pl.pallas_call(
        eighth_kernel,
        grid=(steps,),
        out_shape=[shaped((e_rows + 2, e_cols, HEAD), F32), stats_shape(steps)],
        in_specs=[
            pl.BlockSpec(two, lambda i: (jnp.maximum(i - 1, 0), 0, 0)),
            pl.BlockSpec(two, lambda i: (jnp.minimum(i, steps - 2), 0, 0)),
            halo, halo, weight(1), ANY,
        ],
        out_specs=[pl.BlockSpec((2, e_cols, HEAD), lambda i: (i, 0, 0)), fixed(stats_shape(steps))],
        scratch_shapes=[wide],
        compiler_params=params_of(),
        name="eighth",
    )(eighth, eighth, big_before, big_after, first_weights, y2)
    up_small = jnp.asarray(doubling(t_cols), BF16)
    up_big = jnp.asarray(doubling(s_cols), BF16)
    up_cols = jnp.asarray(doubling(e_cols).T, BF16)
    narrow = pltpu.VMEM((4 * HEAD, 6 * HEAD), BF16)
    y4, y6, pieces = pl.pallas_call(
        between_kernel,
        out_shape=[
            shaped((e_rows + 2, e_cols, HEAD), F32),
            shaped((e_rows + 2, e_cols, HEAD), F32),
            shaped((bands, 16, HEAD), F32),
        ],
        in_specs=[SM] + [VM] * 10,
        out_specs=[VM] * 3,
        scratch_shapes=[
            pltpu.VMEM((e_rows + 4, e_cols, HEAD), BF16),
            pltpu.VMEM((2 * t_rows * bands + 2, 2 * t_cols, HEAD), BF16),
            pltpu.VMEM((2 * t_rows * bands, 2 * t_cols, HEAD), F32),
            pltpu.VMEM((t_rows * bands, 8, 2 * HEAD), F32),
            narrow, narrow, narrow,
        ],
        compiler_params=params_of(),
        name="between",
    )(
        place, got, y2, inner_weights, norm_gain, norm_shift, up_small, up_big,
        stats_early, stats_late, stats_eighth,
    )
    got = everyone(pieces, ROWS)
    classes = class_weight.shape[1]
    class_t = jnp.pad(class_weight.T, ((0, SLOT - classes), (0, 0)))
    class_t3 = jnp.concatenate([class_t] * 3, axis=1)
    out_shape = [shaped((classes, q_rows, q_cols), BF16), shaped((devices, 2, HEAD), F32)]
    args = [got, norm_gain, norm_shift, y0, y1, y4, y6, labels[0], class_t, class_t3, up_cols]
    specs = [fixed(a) for a in args]
    specs[3] = pl.BlockSpec((2, q_cols, HEAD), lambda i: (i, 0, 0))
    logits, pieces = pl.pallas_call(
        final_kernel,
        grid=(pairs,),
        out_shape=out_shape,
        in_specs=[SM, SM] + specs,
        out_specs=[fixed(a) for a in out_shape],
        scratch_shapes=[
            pltpu.VMEM((e_rows + 2, SLOT, e_cols), F32),
            pltpu.VMEM((e_rows + 2, SLOT, q_cols), F32),
            pltpu.VMEM((q_cols // HEAD, q_rows * SLOT, HEAD), F32),
            pltpu.VMEM((8, HEAD), F32),
        ],
        compiler_params=params_of(),
        name="final",
    )(place, class_bias, *args)
    loss_total, valid_count = jnp.sum(everyone(pieces, EVERY), axis=(0, 2))
    mean_loss = loss_total / jnp.maximum(valid_count, 1.0)
    return (logits[None], mean_loss)


def solution(mesh):
    split = Mesh(mesh.devices.reshape(4, 2, 4, 4), ("batch_0", "batch_1", "rows_0", "rows_1"))
    in_specs = (
        P(BATCH, ROWS, None, None),
        P(BATCH, ROWS, None, None),
        P(BATCH, ROWS, None, None),
        P(BATCH, ROWS, None, None),
        P(BATCH, ROWS, None),
        P(),
        P(),
        P(),
        P(),
        P(),
        P(),
    )
    out_specs = (P(BATCH, None, ROWS, None), P())
    return jax.shard_map(
        device_step, mesh=split, in_specs=in_specs, out_specs=out_specs, check_vma=False
    )
```

```python
import jax
import jax.numpy as jnp
import numpy as np
from jax import lax
from jax.experimental import pallas as pl
from jax.experimental.pallas import tpu as pltpu
from jax.sharding import Mesh
from jax.sharding import PartitionSpec as P

GROUP = 4
HEAD = 128
ROWS = ("rows_0", "rows_1")
EVERY = ("batch_0", "batch_1", "rows_0", "rows_1")
BATCH = ("batch_0", "batch_1")
NORM_FLOOR = 0.05
SMALL = (3, 1)
BIG = (1, 2)
STAT_ROWS = 32
SLOT = 32
F32, BF16 = jnp.float32, jnp.bfloat16
VMEM_LIMIT = 60 * 1024 * 1024


def doubling(cols):
    matrix = np.zeros((2 * cols, cols), np.float32)
    for k in range(cols):
        matrix[2 * k, k] += 0.75
        matrix[2 * k, max(k - 1, 0)] += 0.25
        matrix[2 * k + 1, k] += 0.75
        matrix[2 * k + 1, min(k + 1, cols - 1)] += 0.25
    return matrix


def everyone(pieces, axes):
    return lax.all_to_all(pieces, axes, 0, 0)


def matmul(a, b):
    return jnp.dot(a, b, preferred_element_type=F32)


def matmul_t(a, b):
    return lax.dot_general(a, b, (((1,), (1,)), ((), ())), preferred_element_type=F32)


def fill_pair(w_ref, out_ref, depth):
    zero = jnp.zeros((depth, HEAD), BF16)
    for j in range(4):
        for across in range(3):
            rows = slice(j * depth, (j + 1) * depth)
            at = across * 2 * HEAD
            out_ref[rows, at : at + HEAD] = w_ref[j, across] if j < 3 else zero
            out_ref[rows, at + HEAD : at + 2 * HEAD] = w_ref[j - 1, across] if j else zero


def across_taps(z, width, cols):
    pixels = z.shape[0]
    index = lax.broadcasted_iota(jnp.int32, (pixels, width), 0) % cols
    left = jnp.where(index == 0, 0.0, pltpu.roll(z[:, :width], 1, 0))
    right = jnp.where(index == cols - 1, 0.0, pltpu.roll(z[:, 2 * width :], pixels - 1, 0))
    return z[:, width : 2 * width] + left + right


def conv_pair(rows, w_ref):
    return across_taps(matmul(jnp.concatenate(rows, axis=1), w_ref[...]), 2 * HEAD, rows[0].shape[0])


def fill_deep(w_ref, out_ref, depth):
    zero = jnp.zeros((depth, HEAD), BF16)
    for j in range(4):
        rows = slice(j * depth, (j + 1) * depth)
        if j < 3:
            out_ref[rows, :HEAD] = w_ref[j, 0]
            out_ref[rows, HEAD : 2 * HEAD] = w_ref[j, 1]
        out_ref[rows, 2 * HEAD : 3 * HEAD] = w_ref[j, 2] if j < 3 else zero
        out_ref[rows, 3 * HEAD :] = w_ref[j - 1, 2] if j else zero


def conv_deep(rows, w_ref):
    cols, depth = rows[0].shape
    wide = jnp.concatenate(rows, axis=1)
    stacked = jnp.concatenate([wide[:, : 3 * depth], wide[:, depth:]], axis=0)
    near = matmul(stacked, w_ref[: 3 * depth, : 2 * HEAD])
    far = matmul(wide, w_ref[:, 2 * HEAD :])
    taps = [jnp.concatenate([near[:cols, at : at + HEAD], near[cols:, at : at + HEAD]], axis=1) for at in (0, HEAD)]
    index = lax.broadcasted_iota(jnp.int32, far.shape, 0)
    left = jnp.where(index == 0, 0.0, pltpu.roll(taps[0], 1, 0))
    right = jnp.where(index == cols - 1, 0.0, pltpu.roll(far, cols - 1, 0))
    return taps[1] + left + right


def centre(y):
    total = jnp.sum(y, axis=0, keepdims=True)
    centred = y - total * (1.0 / y.shape[0])
    return total, jnp.sum(centred * centred, axis=0, keepdims=True), centred


def sums(y):
    return centre(y)[:2]


def merge(parts, pixels):
    total = sum(p[0] for p in parts)
    mean = total * (1.0 / (pixels * len(parts)))
    square = sum(p[1] + pixels * jnp.square(p[0] * (1.0 / pixels) - mean) for p in parts)
    return total, square


def halves(pair):
    total, square = pair
    return [(total[:, :HEAD], square[:, :HEAD]), (total[:, HEAD:], square[:, HEAD:])]


def group_sum(v):
    lane = lax.broadcasted_iota(jnp.int32, v.shape, 1)
    v = v + jnp.where(lane % 2 == 0, pltpu.roll(v, HEAD - 1, 1), pltpu.roll(v, 1, 1))
    return v + jnp.where(lane % 4 < 2, pltpu.roll(v, HEAD - 2, 1), pltpu.roll(v, 2, 1))


def normed(y, mean, factor, shift):
    return jnp.maximum((y - mean) * factor + shift, 0.0).astype(BF16)


def offset(total, pixels, norm):
    mean, factor, shift = norm
    return (total * (1.0 / pixels) - mean) * factor + shift


def lifted(centred, factor, at):
    return jnp.maximum(centred.astype(F32) * factor + at, 0.0).astype(BF16)


def split_rows(values):
    high = values.astype(BF16).astype(F32)
    rest = values - high
    middle = rest.astype(BF16).astype(F32)
    return [high, middle, rest - middle]


def edges_kernel(quarter, eighth, sixteenth, thirty, small_before, small_after, big_before, big_after, sems):
    copies = []
    groups = (
        (SMALL, (sixteenth, thirty), small_before, small_after),
        (BIG, (quarter, eighth), big_before, big_after),
    )
    for depths, feats, before, after in groups:
        at = 0
        for depth, feat in zip(depths, feats):
            rows, cols, _ = feat.shape
            for i in range(depth):
                spot = pl.ds(at, cols)
                copies.append((feat.at[rows - depth + i], before.at[spot]))
                copies.append((feat.at[i], after.at[spot]))
                at += cols
    started = [pltpu.make_async_copy(a, b, sems.at[i]) for i, (a, b) in enumerate(copies)]
    for copy in started:
        copy.start()
    for copy in started:
        copy.wait()


class Copies:
    def __init__(self, sems):
        self.sems, self.used = sems, 0

    def start(self, source, target):
        copy = pltpu.make_async_copy(source, target, self.sems.at[self.used])
        self.used += 1
        copy.start()
        return copy


def keep_pair(y, field, stats, index, pair):
    total, square, centred = centre(y)
    field[2 * pair] = centred[:, :HEAD].astype(BF16)
    field[2 * pair + 1] = centred[:, HEAD:].astype(BF16)
    stats[index, 0:1] = total
    stats[index, 1:2] = square


def inner_kernel(
    quarter, eighth, weights, _, c0_out, c1_out, stats0, stats1, x0, x1, w0, w1, deep0, deep1, c0, c1, sems
):
    copies = Copies(sems)
    inside = stats0.shape[0]
    wait_w0 = copies.start(weights.at[0], w0)
    rows_of = lambda r, n: copies.start(quarter.at[pl.ds(r, n)], x0.at[pl.ds(r, n)])
    waits = [rows_of(1, 4), rows_of(5, 2)]
    wait_w0.wait()
    fill_deep(w0, deep0, 2 * HEAD)
    out = []
    for i in range(inside):
        p = i + 1
        waits[i].wait()
        if i + 2 < inside:
            waits.append(rows_of(2 * p + 5, 2))
        elif i + 2 == inside:
            wait_w1 = copies.start(weights.at[1], w1)
            wait_x1 = copies.start(eighth, x1)
        rows = [x0[2 * p - 1 + j] for j in range(4)]
        keep_pair(conv_deep(rows, deep0), c0, stats0, i, p)
        out.append(copies.start(c0.at[pl.ds(2 * p, 2)], c0_out.at[pl.ds(2 * p, 2)]))
    wait_w1.wait()
    fill_deep(w1, deep1, 2 * HEAD)
    wait_x1.wait()
    for i in range(stats1.shape[0]):
        p = i + 1
        rows = [x1[2 * i + j] for j in range(4)]
        keep_pair(conv_deep(rows, deep1), c1, stats1, i, p)
        out.append(copies.start(c1.at[pl.ds(2 * p, 2)], c1_out.at[pl.ds(2 * p, 2)]))
    for copy in out:
        copy.wait()


def outer_kernel(
    quarter, eighth, before, after, weights, _, __, c0_out, c1_out, stats0, stats1,
    x0, x1, low, high, w0, w1, deep0, deep1, c0, c1, sems,
):
    copies = Copies(sems)
    q_rows, cols, _ = quarter.shape
    e_rows, e_cols, _ = eighth.shape
    wait_w0 = copies.start(weights.at[0], w0)
    waits = [
        copies.start(before, low),
        copies.start(quarter.at[pl.ds(0, 3)], x0.at[pl.ds(0, 3)]),
        copies.start(after, high),
        copies.start(quarter.at[pl.ds(q_rows - 3, 3)], x0.at[pl.ds(3, 3)]),
    ]
    wait_w1 = copies.start(weights.at[1], w1)
    waits1 = [
        copies.start(eighth.at[pl.ds(0, 2)], x1.at[pl.ds(0, 2)]),
        copies.start(eighth.at[pl.ds(e_rows - 2, 2)], x1.at[pl.ds(2, 2)]),
    ]
    wait_w0.wait()
    fill_deep(w0, deep0, 2 * HEAD)
    out = []
    for i in range(2):
        waits[2 * i].wait()
        waits[2 * i + 1].wait()
        rows = [x0[3 * i + j] for j in range(3)]
        rows = rows + [high[:cols]] if i else [low[:cols]] + rows
        keep_pair(conv_deep(rows, deep0), c0, stats0, i, i)
        spot = pl.ds(i * (q_rows - 2), 2)
        out.append(copies.start(c0.at[pl.ds(2 * i, 2)], c0_out.at[spot]))
    wait_w1.wait()
    fill_deep(w1, deep1, 2 * HEAD)
    for i in range(2):
        waits1[i].wait()
        halo = (high if i else low)
        rows = [x1[2 * i + j] for j in range(2)]
        extra = [halo[cols + j * e_cols : cols + (j + 1) * e_cols] for j in range(2)]
        rows = rows + extra if i else extra + rows
        keep_pair(conv_deep(rows, deep1), c1, stats1, i, i)
        spot = pl.ds(i * e_rows, 2)
        out.append(copies.start(c1.at[pl.ds(2 * i, 2)], c1_out.at[spot]))
    for copy in out:
        copy.wait()


def coarse_kernel(before, after, sixteenth, thirty, w2, w3, y2, pieces, wide2, wide3):
    depth = 2 * HEAD
    fill_deep(w2, wide2, depth)
    fill_deep(w3, wide3, depth)
    own, cols, _ = sixteenth.shape
    ring = SMALL[0]
    rows = [before[i * cols : (i + 1) * cols] for i in range(ring)]
    rows += [sixteenth[i] for i in range(own)]
    rows += [after[i * cols : (i + 1) * cols] for i in range(ring)]
    parts = []
    for p in range(y2.shape[0] // 2):
        out = conv_deep(rows[2 * p : 2 * p + 4], wide2)
        y2[2 * p] = out[:, :HEAD]
        y2[2 * p + 1] = out[:, HEAD:]
        if 0 < p < y2.shape[0] // 2 - 1:
            parts += halves(sums(out))
    at = ring * cols
    out = conv_deep([before[at:], thirty[0], thirty[1], after[at:]], wide3)
    total3, square3, coarse = centre(jnp.concatenate([out[:, :HEAD], out[:, HEAD:]], axis=0))
    coarse = coarse.astype(BF16)
    total, square = merge(parts, cols)
    values = jnp.concatenate([total, square, total3, square3, jnp.zeros((4, HEAD), F32)], axis=0)
    head = jnp.concatenate(split_rows(values) + [jnp.zeros((8, HEAD), F32)], axis=0).astype(BF16)
    for i in range(pieces.shape[0]):
        pieces[i, :STAT_ROWS] = head
        pieces[i, STAT_ROWS:] = coarse


def between_kernel(
    place, got, y2_in, weights_in, gain, shift, up_small, up_big, inner0, outer0, inner1, outer1,
    c4_out, c6_out, stats4, stats6, pieces,
    y2, weights, c4, c6, fine, coarse, field5, stats5, wide0, wide1, wide2, sems,
):
    members = got.shape[0]
    position = place[0]
    first, last = position == 0, position == members - 1
    copies = Copies(sems)
    wait_w = copies.start(weights_in, weights)
    wait_y2 = copies.start(y2_in, y2)
    out = []

    def merged_norm(each, pixels, layer):
        count = pixels * len(each) * GROUP
        mean = group_sum(jnp.broadcast_to(sum(p[0] for p in each), (8, HEAD)))[0:1] * (1.0 / count)
        square = sum(p[1] + pixels * jnp.square(p[0] * (1.0 / pixels) - mean) for p in each)
        var = group_sum(jnp.broadcast_to(square, (8, HEAD)))[0:1] * (1.0 / count)
        return mean, gain[layer : layer + 1] * lax.rsqrt(var + NORM_FLOOR), shift[layer : layer + 1]

    def up_conv(acts, wide, kept, kept_out, stats):
        count = len(acts)
        doubled = []
        for k in range(0, count, 2):
            both = matmul(up_big[...], jnp.concatenate([acts[k], acts[k + 1]], axis=1))
            doubled += [both[:, :HEAD], both[:, HEAD:]]
        lines = 2 * (count - 2)
        for k in range(1, count - 1):
            for half, other in ((0, k - 1), (1, k + 1)):
                line = 0.75 * doubled[k] + 0.25 * doubled[other]
                at = 2 * (k - 1) + half
                if at < 2:
                    line = jnp.where(first, 0.0, line)
                if at >= lines - 2:
                    line = jnp.where(last, 0.0, line)
                fine[at] = line.astype(BF16)
        own = []
        for p in range(lines // 2 - 1):
            keep_pair(conv_pair([fine[2 * p + j] for j in range(4)], wide), kept, stats, p, p)
            span = pl.ds(2 * p, 2)
            out.append(copies.start(kept.at[span], kept_out.at[span]))
            two = halves((stats[p, 0:1], stats[p, 1:2]))
            own += two[1:] if p == 0 else two[:1] if p == lines // 2 - 2 else two
        return merge(own, kept.shape[1])

    lines, cols = coarse.shape[0] - 2, coarse.shape[1]
    small = cols // 2
    blocks = [got[i, :STAT_ROWS].astype(F32) for i in range(members)]
    blocks = [b[0:8] + b[8:16] + b[16:24] for b in blocks]
    norm3 = merged_norm([(b[2:3], b[3:4]) for b in blocks], 2 * small, 3)
    doubled = []
    for i in range(members):
        a = lifted(got[i, STAT_ROWS:], norm3[1], offset(blocks[i][2:3], 2 * small, norm3))
        both = matmul(up_small[...], jnp.concatenate([a[:small], a[small:]], axis=1))
        doubled += [both[:, :HEAD], both[:, HEAD:]]
    coarse[0] = jnp.zeros((cols, HEAD), BF16)
    coarse[lines + 1] = jnp.zeros((cols, HEAD), BF16)
    for k in range(len(doubled)):
        for half, other in ((0, max(k - 1, 0)), (1, min(k + 1, len(doubled) - 1))):
            coarse[1 + 2 * k + half] = (0.75 * doubled[k] + 0.25 * doubled[other]).astype(BF16)
    wait_w.wait()
    for i, wide in enumerate((wide0, wide1, wide2)):
        fill_pair(weights.at[i], wide, HEAD)
    fold = 4

    def step(q, carry):
        base = q * (2 * fold)
        lhs = jnp.concatenate(
            [
                jnp.concatenate([coarse[base + 2 * i + j] for j in range(4)], axis=1)
                for i in range(fold)
            ],
            axis=0,
        )
        y = across_taps(matmul(lhs, wide1[...]), 2 * HEAD, cols)
        for i in range(fold):
            field5[base + 2 * i] = y[i * cols : (i + 1) * cols, :HEAD]
            field5[base + 2 * i + 1] = y[i * cols : (i + 1) * cols, HEAD:]
        total, square = sums(y)
        stats5[q, 0:1] = total
        stats5[q, 1:2] = square
        return carry

    lax.fori_loop(0, lines // (2 * fold), step, 0, unroll=2)
    wait_y2.wait()
    norm2 = merged_norm([(b[0:1], b[1:2]) for b in blocks], y2.shape[1] * (y2.shape[0] - 4), 2)
    acts = [normed(y2[i], *norm2) for i in range(y2.shape[0])]
    count = len(acts)
    acts[1] = jnp.where(first, acts[2], acts[1])
    acts[count - 2] = jnp.where(last, acts[count - 3], acts[count - 2])
    merged4 = up_conv(acts, wide0, c4, c4_out, stats4)
    parts5 = []
    for q in range(lines // (2 * fold)):
        parts5 += halves((stats5[q, 0:1], stats5[q, 1:2]))
    norm5 = merged_norm(parts5, cols * fold, 5)
    band = lines // members
    acts = []
    for i in range(band + 4):
        at = jnp.clip(position * band + (i - 2), 0, lines - 1)
        acts.append(normed(field5[at], *norm5))
    merged6 = up_conv(acts, wide2, c6, c6_out, stats6)
    parts0, parts1 = [], []
    for stats in (inner0, outer0):
        for p in range(stats.shape[0]):
            parts0 += halves((stats[p, 0:1], stats[p, 1:2]))
    for p in range(inner1.shape[0]):
        parts1 += halves((inner1[p, 0:1], inner1[p, 1:2]))
    for p in range(2):
        parts1.append(halves((outer1[p, 0:1], outer1[p, 1:2]))[1 - p])
    eighth_cols = c4.shape[1]
    merged = [merge(parts0, 2 * eighth_cols), merge(parts1, eighth_cols), merged4, merged6]
    pad = [jnp.zeros((4, HEAD), F32)]
    block = jnp.concatenate([m[0] for m in merged] + pad + [m[1] for m in merged] + pad, axis=0)
    for i in range(members):
        pieces[i] = block
    for copy in out:
        copy.wait()


def final_kernel(
    place, bias, got, gain, shift, inner0, outer0, inner1, outer1, stats4, stats6, labels, class_t, class_t3, up_cols,
    c0_in, c1_in, c4_in, c6_in, logits, pieces, c0, c1, c4, c6, lines, doubled, scores, sems,
):
    members = got.shape[0]
    copies = Copies(sems)
    waits = [copies.start(a, b) for a, b in ((c1_in, c1), (c4_in, c4), (c6_in, c6))]
    rows = c0.shape[0]
    chunk = rows // 4
    waits0 = [
        copies.start(c0_in.at[pl.ds(i * chunk, chunk)], c0.at[pl.ds(i * chunk, chunk)]) for i in range(4)
    ]
    count = c4.shape[0]
    first, last = place[0] == 0, place[0] == members - 1
    row = lax.broadcasted_iota(jnp.int32, (8, HEAD), 0)
    own = float((count - 2) * c4.shape[1])
    pixels = jnp.where(row == 0, 4.0 * own, own)
    total = sum(got[i, 0:8] for i in range(members))
    mean = group_sum(total) / (pixels * (members * GROUP))
    square = sum(got[i, 8:16] + pixels * jnp.square(got[i, 0:8] / pixels - mean) for i in range(members))
    scale = lax.rsqrt(group_sum(square) / (pixels * (members * GROUP)) + NORM_FLOOR)
    norms = [
        (mean[j : j + 1], gain[layer : layer + 1] * scale[j : j + 1], shift[layer : layer + 1])
        for j, layer in enumerate((0, 1, 4, 6))
    ]

    def lift(field, r, total, norm):
        half = total[:, (r % 2) * HEAD : (r % 2 + 1) * HEAD]
        return lifted(field[r], norm[1], offset(half, field.shape[1], norm))

    def joined(inner, outer):
        pairs = [inner[p, 0:1] for p in range(inner.shape[0])]
        return [outer[0, 0:1]] + pairs + [outer[1, 0:1]]

    totals0, totals1 = joined(inner0, outer0), joined(inner1, outer1)
    for wait in waits:
        wait.wait()
    for i in range(count):
        p = i // 2
        acts = [
            lift(c1, i, totals1[p], norms[1]),
            lift(c4, i, stats4[p, 0:1], norms[2]),
            lift(c6, i, stats6[p, 0:1], norms[3]),
        ]
        lines[i] = matmul_t(class_t3[...], jnp.concatenate(acts, axis=1))
    lines[0] = jnp.where(first, lines[1], lines[0])
    lines[count - 1] = jnp.where(last, lines[count - 2], lines[count - 1])
    for i in range(count):
        value = lines[i]
        high = value.astype(BF16)
        low = (value - high.astype(F32)).astype(BF16)
        both = matmul(jnp.concatenate([high, low], axis=0), up_cols[...])
        doubled[i] = both[:SLOT] + both[SLOT:]
    for r in range(rows):
        if r % chunk == 0:
            waits0[r // chunk].wait()
        p = r // 2
        value = matmul_t(class_t[...], lift(c0, r, totals0[p], norms[0]))
        value = value + (0.75 * doubled[p + 1] + 0.25 * doubled[p + 2 * (r % 2)])
        for i in range(scores.shape[0]):
            scores[i, r * SLOT : (r + 1) * SLOT] = value[:, i * HEAD : (i + 1) * HEAD]
    label_map = labels[...]
    exps = jnp.zeros(label_map.shape, F32)
    picked = jnp.zeros(label_map.shape, F32)
    for c in range(logits.shape[0]):
        tiles = [scores.at[i][pl.ds(c, rows, stride=SLOT), :] for i in range(scores.shape[0])]
        score = jnp.concatenate(tiles, axis=1) + bias[c]
        logits[c] = score.astype(BF16)
        exps = exps + jnp.exp(score)
        picked = picked + jnp.where(label_map == c, score, 0.0)
    usable = label_map != 255
    terms = jnp.where(usable, jnp.log(exps) - picked, 0.0)
    counts = jnp.where(usable, 1.0, 0.0)
    out = []
    for v in (terms, counts):
        v = jnp.sum(v, axis=0, keepdims=True)
        out.append(sum(v[:, i * HEAD : (i + 1) * HEAD] for i in range(v.shape[1] // HEAD)))
    both = jnp.concatenate(out, axis=0)
    for i in range(pieces.shape[0]):
        pieces[i] = both


def params_of(**kw):
    return pltpu.CompilerParams(vmem_limit_bytes=VMEM_LIMIT, **kw)


def shaped(shape, dtype):
    return jax.ShapeDtypeStruct(shape, dtype)


VM = pl.BlockSpec(memory_space=pltpu.VMEM)
SM = pl.BlockSpec(memory_space=pltpu.SMEM)
ANY = pl.BlockSpec(memory_space=pl.ANY)


def device_step(
    feat_quarter,
    feat_eighth,
    feat_sixteenth,
    feat_thirty,
    labels,
    first_weights,
    inner_weights,
    norm_gain,
    norm_shift,
    class_weight,
    class_bias,
):
    position = lax.axis_index(ROWS)
    bands = lax.axis_size(ROWS)
    devices = bands * lax.axis_size(BATCH)
    place = position.astype(jnp.int32).reshape(1)
    up_pairs = [(i, i + 1) for i in range(bands - 1)]
    down_pairs = [(j, i) for i, j in up_pairs]
    feats = [feat_quarter[0], feat_eighth[0], feat_sixteenth[0], feat_thirty[0]]
    quarter, eighth, sixteenth, thirty = feats
    q_rows, q_cols, depth = quarter.shape
    e_rows, e_cols, _ = eighth.shape
    s_rows, s_cols, _ = sixteenth.shape
    t_rows, t_cols, _ = thirty.shape
    small = shaped((SMALL[0] * s_cols + SMALL[1] * t_cols, depth), BF16)
    big = shaped((BIG[0] * q_cols + BIG[1] * e_cols, depth), BF16)
    small_before, small_after, big_before, big_after = pl.pallas_call(
        edges_kernel,
        out_shape=[small, small, big, big],
        in_specs=[ANY] * 4,
        out_specs=[VM] * 4,
        scratch_shapes=[pltpu.SemaphoreType.DMA((2 * (sum(SMALL) + sum(BIG)),))],
        compiler_params=params_of(),
        name="edges",
    )(*feats)
    small_before = lax.ppermute(small_before, ROWS, up_pairs)
    small_after = lax.ppermute(small_after, ROWS, down_pairs)
    big_before = lax.ppermute(big_before, ROWS, up_pairs)
    big_after = lax.ppermute(big_after, ROWS, down_pairs)

    def fixed(a, *index):
        index = index or (0,) * len(a.shape)
        return pl.BlockSpec(a.shape, lambda i: index)

    def weight(level):
        return pl.BlockSpec((None,) + first_weights.shape[1:], lambda i: (level, 0, 0, 0, 0))

    deep = pltpu.VMEM((4 * depth, 4 * HEAD), BF16)
    raw = pltpu.VMEM(first_weights.shape[1:], BF16)
    pairs = q_rows // 2
    steps = e_rows // 2 + 1
    field0 = shaped((q_rows, q_cols, HEAD), BF16)
    field1 = shaped((e_rows + 2, e_cols, HEAD), BF16)
    stats_shape = lambda n: shaped((n, 8, 2 * HEAD), F32)
    room = lambda a: pltpu.VMEM(a.shape, a.dtype)
    piece = shaped((bands, STAT_ROWS + t_rows * t_cols, HEAD), BF16)
    y2_shape = shaped((s_rows + 4, s_cols, HEAD), F32)
    coarse_call = pl.pallas_call(
        coarse_kernel,
        grid=(1,),
        out_shape=[y2_shape, piece],
        in_specs=[fixed(small), fixed(small), fixed(sixteenth), fixed(thirty), weight(2), weight(3)],
        out_specs=[fixed(y2_shape), fixed(piece)],
        scratch_shapes=[deep, deep],
        compiler_params=params_of(),
        name="coarse",
    )
    y2, pieces = coarse_call(
        small_before, small_after, sixteenth, thirty, first_weights, first_weights
    )
    got = everyone(pieces, ROWS)
    inside0, inside1 = pairs - 2, steps - 2
    c0, c1, inner0, inner1 = pl.pallas_call(
        inner_kernel,
        out_shape=[field0, field1, stats_shape(inside0), stats_shape(inside1)],
        in_specs=[ANY] * 4,
        out_specs=[ANY, ANY, VM, VM],
        scratch_shapes=[
            room(quarter), room(eighth), raw, raw, deep, deep, room(field0), room(field1),
            pltpu.SemaphoreType.DMA((2 * inside0 + inside1 + 3,)),
        ],
        compiler_params=params_of(),
        name="inner",
    )(quarter, eighth, first_weights, y2)
    c0, c1, outer0, outer1 = pl.pallas_call(
        outer_kernel,
        out_shape=[field0, field1, stats_shape(2), stats_shape(2)],
        in_specs=[ANY] * 7,
        out_specs=[ANY, ANY, VM, VM],
        input_output_aliases={5: 0, 6: 1},
        scratch_shapes=[
            pltpu.VMEM((6, q_cols, depth), BF16), pltpu.VMEM((4, e_cols, depth), BF16), room(big), room(big),
            raw, raw, deep, deep,
            pltpu.VMEM((4, q_cols, HEAD), BF16), pltpu.VMEM((4, e_cols, HEAD), BF16),
            pltpu.SemaphoreType.DMA((12,)),
        ],
        compiler_params=params_of(),
        name="outer",
    )(quarter, eighth, big_before, big_after, first_weights, c0, c1)
    up_small = jnp.asarray(doubling(t_cols), BF16)
    up_big = jnp.asarray(doubling(s_cols), BF16)
    up_cols = jnp.asarray(doubling(e_cols).T, BF16)
    narrow = pltpu.VMEM((4 * HEAD, 6 * HEAD), BF16)
    c4, c6, stats4, stats6, pieces = pl.pallas_call(
        between_kernel,
        out_shape=[field1, field1, stats_shape(steps), stats_shape(steps), shaped((bands, 16, HEAD), F32)],
        in_specs=[SM, VM, ANY, ANY] + [VM] * 8,
        out_specs=[ANY, ANY, VM, VM, VM],
        scratch_shapes=[
            room(y2), room(inner_weights), room(field1), room(field1),
            pltpu.VMEM((e_rows + 4, e_cols, HEAD), BF16),
            pltpu.VMEM((2 * t_rows * bands + 2, 2 * t_cols, HEAD), BF16),
            pltpu.VMEM((2 * t_rows * bands, 2 * t_cols, HEAD), F32),
            pltpu.VMEM((t_rows * bands, 8, 2 * HEAD), F32),
            narrow, narrow, narrow,
            pltpu.SemaphoreType.DMA((2 * steps + 2,)),
        ],
        compiler_params=params_of(),
        name="between",
    )(
        place, got, y2, inner_weights, norm_gain, norm_shift, up_small, up_big,
        inner0, outer0, inner1, outer1,
    )
    got = everyone(pieces, ROWS)
    classes = class_weight.shape[1]
    class_t = jnp.pad(class_weight.T, ((0, SLOT - classes), (0, 0)))
    class_t3 = jnp.concatenate([class_t] * 3, axis=1)
    logits, pieces = pl.pallas_call(
        final_kernel,
        out_shape=[shaped((classes, q_rows, q_cols), BF16), shaped((devices, 2, HEAD), F32)],
        in_specs=[SM, SM] + [VM] * 13 + [ANY] * 4,
        out_specs=[VM, VM],
        scratch_shapes=[
            room(field0), room(field1), room(field1), room(field1),
            pltpu.VMEM((e_rows + 2, SLOT, e_cols), F32),
            pltpu.VMEM((e_rows + 2, SLOT, q_cols), F32),
            pltpu.VMEM((q_cols // HEAD, q_rows * SLOT, HEAD), F32),
            pltpu.SemaphoreType.DMA((7,)),
        ],
        compiler_params=params_of(),
        name="final",
    )(
        place, class_bias, got, norm_gain, norm_shift, inner0, outer0, inner1, outer1, stats4, stats6,
        labels[0], class_t, class_t3, up_cols, c0, c1, c4, c6,
    )
    loss_total, valid_count = jnp.sum(everyone(pieces, EVERY), axis=(0, 2))
    mean_loss = loss_total / jnp.maximum(valid_count, 1.0)
    return (logits[None], mean_loss)


def solution(mesh):
    split = Mesh(mesh.devices.reshape(4, 2, 4, 4), ("batch_0", "batch_1", "rows_0", "rows_1"))
    in_specs = (
        P(BATCH, ROWS, None, None),
        P(BATCH, ROWS, None, None),
        P(BATCH, ROWS, None, None),
        P(BATCH, ROWS, None, None),
        P(BATCH, ROWS, None),
        P(),
        P(),
        P(),
        P(),
        P(),
        P(),
    )
    out_specs = (P(BATCH, None, ROWS, None), P())
    return jax.shard_map(device_step, mesh=split, in_specs=in_specs, out_specs=out_specs, check_vma=False)
```

```python
import jax
import jax.numpy as jnp
import numpy as np
from jax import lax
from jax.experimental import pallas as pl
from jax.experimental.pallas import tpu as pltpu
from jax.sharding import Mesh
from jax.sharding import PartitionSpec as P

GROUP = 4
HEAD = 128
ROWS = ("rows_0", "rows_1")
EVERY = ("batch_0", "batch_1", "rows_0", "rows_1")
BATCH = ("batch_0", "batch_1")
NORM_FLOOR = 0.05
SMALL = (3, 1)
BIG = (1, 2)
STAT_ROWS = 16
SLOT = 32
F32, BF16 = jnp.float32, jnp.bfloat16
VMEM_LIMIT = 60 * 1024 * 1024


def doubling(cols):
    matrix = np.zeros((2 * cols, cols), np.float32)
    for k in range(cols):
        matrix[2 * k, k] += 0.75
        matrix[2 * k, max(k - 1, 0)] += 0.25
        matrix[2 * k + 1, k] += 0.75
        matrix[2 * k + 1, min(k + 1, cols - 1)] += 0.25
    return matrix


def everyone(pieces, axes):
    return lax.all_to_all(pieces, axes, 0, 0)


def matmul(a, b):
    return jnp.dot(a, b, preferred_element_type=F32)


def matmul_t(a, b):
    return lax.dot_general(a, b, (((1,), (1,)), ((), ())), preferred_element_type=F32)


def fill_pair(w_ref, out_ref, depth):
    zero = jnp.zeros((depth, HEAD), BF16)
    for j in range(4):
        for across in range(3):
            rows = slice(j * depth, (j + 1) * depth)
            at = across * 2 * HEAD
            out_ref[rows, at : at + HEAD] = w_ref[j, across] if j < 3 else zero
            out_ref[rows, at + HEAD : at + 2 * HEAD] = w_ref[j - 1, across] if j else zero


def across_taps(z, width, cols):
    pixels = z.shape[0]
    index = lax.broadcasted_iota(jnp.int32, (pixels, width), 0) % cols
    left = jnp.where(index == 0, 0.0, pltpu.roll(z[:, :width], 1, 0))
    right = jnp.where(index == cols - 1, 0.0, pltpu.roll(z[:, 2 * width :], pixels - 1, 0))
    return z[:, width : 2 * width] + left + right


def conv_pair(rows, w_ref):
    return across_taps(matmul(jnp.concatenate(rows, axis=1), w_ref[...]), 2 * HEAD, rows[0].shape[0])


def fill_deep(w_ref, out_ref, depth):
    zero = jnp.zeros((depth, HEAD), BF16)
    for j in range(4):
        rows = slice(j * depth, (j + 1) * depth)
        if j < 3:
            out_ref[rows, :HEAD] = w_ref[j, 0]
            out_ref[rows, HEAD : 2 * HEAD] = w_ref[j, 1]
        out_ref[rows, 2 * HEAD : 3 * HEAD] = w_ref[j, 2] if j < 3 else zero
        out_ref[rows, 3 * HEAD :] = w_ref[j - 1, 2] if j else zero


def conv_deep(rows, w_ref):
    cols, depth = rows[0].shape
    wide = jnp.concatenate(rows, axis=1)
    stacked = jnp.concatenate([wide[:, : 3 * depth], wide[:, depth:]], axis=0)
    near = matmul(stacked, w_ref[: 3 * depth, : 2 * HEAD])
    far = matmul(wide, w_ref[:, 2 * HEAD :])
    taps = [jnp.concatenate([near[:cols, at : at + HEAD], near[cols:, at : at + HEAD]], axis=1) for at in (0, HEAD)]
    index = lax.broadcasted_iota(jnp.int32, far.shape, 0)
    left = jnp.where(index == 0, 0.0, pltpu.roll(taps[0], 1, 0))
    right = jnp.where(index == cols - 1, 0.0, pltpu.roll(far, cols - 1, 0))
    return taps[1] + left + right


def centre(y):
    total = jnp.sum(y, axis=0, keepdims=True)
    centred = y - total * (1.0 / y.shape[0])
    return total, jnp.sum(centred * centred, axis=0, keepdims=True), centred


def sums(y):
    return centre(y)[:2]


def merge(parts, pixels):
    total = sum(p[0] for p in parts)
    mean = total * (1.0 / (pixels * len(parts)))
    square = sum(p[1] + pixels * jnp.square(p[0] * (1.0 / pixels) - mean) for p in parts)
    return total, square


def halves(pair):
    total, square = pair
    return [(total[:, :HEAD], square[:, :HEAD]), (total[:, HEAD:], square[:, HEAD:])]


def group_sum(v):
    lane = lax.broadcasted_iota(jnp.int32, v.shape, 1)
    v = v + jnp.where(lane % 2 == 0, pltpu.roll(v, HEAD - 1, 1), pltpu.roll(v, 1, 1))
    return v + jnp.where(lane % 4 < 2, pltpu.roll(v, HEAD - 2, 1), pltpu.roll(v, 2, 1))


def normed(y, mean, factor, shift):
    return jnp.maximum((y - mean) * factor + shift, 0.0).astype(BF16)


def offset(total, pixels, norm):
    mean, factor, shift = norm
    return (total * (1.0 / pixels) - mean) * factor + shift


def lifted(centred, factor, at):
    return jnp.maximum(centred.astype(F32) * factor + at, 0.0).astype(BF16)


def split_rows(values):
    high = values.astype(BF16).astype(F32)
    rest = values - high
    middle = rest.astype(BF16).astype(F32)
    return [high, middle, rest - middle]


def edges_kernel(quarter, eighth, sixteenth, thirty, small_before, small_after, big_before, big_after, sems):
    copies = []
    groups = (
        (SMALL, (sixteenth, thirty), small_before, small_after),
        (BIG, (quarter, eighth), big_before, big_after),
    )
    for depths, feats, before, after in groups:
        at = 0
        for depth, feat in zip(depths, feats):
            rows, cols, _ = feat.shape
            for i in range(depth):
                spot = pl.ds(at, cols)
                copies.append((feat.at[rows - depth + i], before.at[spot]))
                copies.append((feat.at[i], after.at[spot]))
                at += cols
    started = [pltpu.make_async_copy(a, b, sems.at[i]) for i, (a, b) in enumerate(copies)]
    for copy in started:
        copy.start()
    for copy in started:
        copy.wait()


class Copies:
    def __init__(self, sems):
        self.sems, self.used = sems, 0

    def start(self, source, target):
        copy = pltpu.make_async_copy(source, target, self.sems.at[self.used])
        self.used += 1
        copy.start()
        return copy


def keep_pair(y, field, stats, index, pair):
    total, square, centred = centre(y)
    field[2 * pair] = centred[:, :HEAD].astype(BF16)
    field[2 * pair + 1] = centred[:, HEAD:].astype(BF16)
    stats[index, 0:1] = total
    stats[index, 1:2] = square


def inner_kernel(
    quarter, eighth, weights, _, c0_out, c1_out, stats0, stats1, x0, x1, w0, w1, deep0, deep1, c0, c1, sems
):
    copies = Copies(sems)
    rows0 = pl.ds(1, quarter.shape[0] - 2)
    waits1 = [copies.start(weights.at[1], w1), copies.start(eighth, x1)]
    waits0 = [copies.start(weights.at[0], w0), copies.start(quarter.at[rows0], x0.at[rows0])]
    out = []
    for wait in waits1:
        wait.wait()
    fill_deep(w1, deep1, 2 * HEAD)
    for i in range(stats1.shape[0]):
        p = i + 1
        keep_pair(conv_deep([x1[2 * i + j] for j in range(4)], deep1), c1, stats1, i, p)
        out.append(copies.start(c1.at[pl.ds(2 * p, 2)], c1_out.at[pl.ds(2 * p, 2)]))
    for wait in waits0:
        wait.wait()
    fill_deep(w0, deep0, 2 * HEAD)
    for i in range(stats0.shape[0]):
        p = i + 1
        keep_pair(conv_deep([x0[2 * i + 1 + j] for j in range(4)], deep0), c0, stats0, i, p)
        out.append(copies.start(c0.at[pl.ds(2 * p, 2)], c0_out.at[pl.ds(2 * p, 2)]))
    for copy in out:
        copy.wait()


class Outer:
    def __init__(self, copies, inputs, outputs, room):
        self.copies, self.outputs, self.room = copies, outputs, room
        quarter, eighth, before, after, weights = inputs
        x0, x1, low, high, w0, w1 = room[:6]
        self.q_rows, self.cols, _ = quarter.shape
        self.e_rows, self.e_cols, _ = eighth.shape
        pairs = (
            (weights.at[1], w1),
            (weights.at[0], w0),
            (before, low),
            (after, high),
            (eighth.at[pl.ds(0, 2)], x1.at[pl.ds(0, 2)]),
            (eighth.at[pl.ds(self.e_rows - 2, 2)], x1.at[pl.ds(2, 2)]),
            (quarter.at[pl.ds(0, 3)], x0.at[pl.ds(0, 3)]),
            (quarter.at[pl.ds(self.q_rows - 3, 3)], x0.at[pl.ds(3, 3)]),
        )
        self.waits = [copies.start(*pair) for pair in pairs]

    def work(self):
        for wait in self.waits:
            wait.wait()
        c0_out, c1_out, stats0, stats1 = self.outputs
        x0, x1, low, high, w0, w1, deep0, deep1, c0, c1 = self.room
        fill_deep(w1, deep1, 2 * HEAD)
        fill_deep(w0, deep0, 2 * HEAD)
        cols, e_cols = self.cols, self.e_cols
        for i in range(2):
            rows = [x0[3 * i + j] for j in range(3)]
            keep_pair(conv_deep(rows + [high[:cols]] if i else [low[:cols]] + rows, deep0), c0, stats0, i, i)
        for i in range(2):
            halo = high if i else low
            rows = [x1[2 * i + j] for j in range(2)]
            extra = [halo[cols + j * e_cols : cols + (j + 1) * e_cols] for j in range(2)]
            keep_pair(conv_deep(rows + extra if i else extra + rows, deep1), c1, stats1, i, i)
        out = []
        for i in range(2):
            spot = pl.ds(2 * i, 2)
            out.append(self.copies.start(c0.at[spot], c0_out.at[pl.ds(i * (self.q_rows - 2), 2)]))
            out.append(self.copies.start(c1.at[spot], c1_out.at[pl.ds(i * self.e_rows, 2)]))
        return out


def coarse_kernel(before, after, sixteenth, thirty, w2, w3, y2, pieces, wide2, wide3):
    depth = 2 * HEAD
    fill_deep(w2, wide2, depth)
    fill_deep(w3, wide3, depth)
    own, cols, _ = sixteenth.shape
    ring = SMALL[0]
    rows = [before[i * cols : (i + 1) * cols] for i in range(ring)]
    rows += [sixteenth[i] for i in range(own)]
    rows += [after[i * cols : (i + 1) * cols] for i in range(ring)]
    parts = []
    for p in range(y2.shape[0] // 2):
        out = conv_deep(rows[2 * p : 2 * p + 4], wide2)
        y2[2 * p] = out[:, :HEAD]
        y2[2 * p + 1] = out[:, HEAD:]
        if 0 < p < y2.shape[0] // 2 - 1:
            parts += halves(sums(out))
    at = ring * cols
    out = conv_deep([before[at:], thirty[0], thirty[1], after[at:]], wide3)
    total3, square3, coarse = centre(jnp.concatenate([out[:, :HEAD], out[:, HEAD:]], axis=0))
    coarse = coarse.astype(BF16)
    total, square = merge(parts, cols)
    values = jnp.concatenate([total, square, total3, square3], axis=0)
    head = jnp.concatenate(split_rows(values) + [jnp.zeros((4, HEAD), F32)], axis=0).astype(BF16)
    for i in range(pieces.shape[0]):
        pieces[i, :STAT_ROWS] = head
        pieces[i, STAT_ROWS:] = coarse


def between_kernel(
    place, got, y2_in, weights_in, gain, shift, up_small, up_big, inner0, inner1,
    quarter, eighth, before, after, first_weights, _, __,
    c0_out, c1_out, outer0, outer1, c4_out, c6_out, stats4, stats6, pieces,
    y2, weights, c4, c6, fine, coarse, field5, stats5, wide0, wide1, wide2, sems, *room,
):
    members = got.shape[0]
    position = place[0]
    first, last = position == 0, position == members - 1
    copies = Copies(sems)
    wait_w = copies.start(weights_in, weights)
    wait_y2 = copies.start(y2_in, y2)
    outer = Outer(
        copies, (quarter, eighth, before, after, first_weights), (c0_out, c1_out, outer0, outer1), room
    )
    out = []

    def merged_norm(each, pixels, layer):
        count = pixels * len(each) * GROUP
        mean = group_sum(jnp.broadcast_to(sum(p[0] for p in each), (8, HEAD)))[0:1] * (1.0 / count)
        square = sum(p[1] + pixels * jnp.square(p[0] * (1.0 / pixels) - mean) for p in each)
        var = group_sum(jnp.broadcast_to(square, (8, HEAD)))[0:1] * (1.0 / count)
        return mean, gain[layer : layer + 1] * lax.rsqrt(var + NORM_FLOOR), shift[layer : layer + 1]

    def up_conv(acts, wide, kept, kept_out, stats):
        count = len(acts)
        doubled = []
        for k in range(0, count, 2):
            both = matmul(up_big[...], jnp.concatenate([acts[k], acts[k + 1]], axis=1))
            doubled += [both[:, :HEAD], both[:, HEAD:]]
        lines = 2 * (count - 2)
        for k in range(1, count - 1):
            for half, other in ((0, k - 1), (1, k + 1)):
                line = 0.75 * doubled[k] + 0.25 * doubled[other]
                at = 2 * (k - 1) + half
                if at < 2:
                    line = jnp.where(first, 0.0, line)
                if at >= lines - 2:
                    line = jnp.where(last, 0.0, line)
                fine[at] = line.astype(BF16)
        own = []
        for p in range(lines // 2 - 1):
            keep_pair(conv_pair([fine[2 * p + j] for j in range(4)], wide), kept, stats, p, p)
            span = pl.ds(2 * p, 2)
            out.append(copies.start(kept.at[span], kept_out.at[span]))
            two = halves((stats[p, 0:1], stats[p, 1:2]))
            own += two[1:] if p == 0 else two[:1] if p == lines // 2 - 2 else two
        return merge(own, kept.shape[1])

    lines, cols = coarse.shape[0] - 2, coarse.shape[1]
    small = cols // 2
    blocks = [got[i, :STAT_ROWS].astype(F32) for i in range(members)]
    blocks = [b[0:4] + b[4:8] + b[8:12] for b in blocks]
    norm3 = merged_norm([(b[2:3], b[3:4]) for b in blocks], 2 * small, 3)
    doubled = []
    for i in range(members):
        a = lifted(got[i, STAT_ROWS:], norm3[1], offset(blocks[i][2:3], 2 * small, norm3))
        both = matmul(up_small[...], jnp.concatenate([a[:small], a[small:]], axis=1))
        doubled += [both[:, :HEAD], both[:, HEAD:]]
    coarse[0] = jnp.zeros((cols, HEAD), BF16)
    coarse[lines + 1] = jnp.zeros((cols, HEAD), BF16)
    for k in range(len(doubled)):
        for half, other in ((0, max(k - 1, 0)), (1, min(k + 1, len(doubled) - 1))):
            coarse[1 + 2 * k + half] = (0.75 * doubled[k] + 0.25 * doubled[other]).astype(BF16)
    wait_w.wait()
    for i, wide in enumerate((wide0, wide1, wide2)):
        fill_pair(weights.at[i], wide, HEAD)
    fold = 4

    def step(q, carry):
        base = q * (2 * fold)
        lhs = jnp.concatenate(
            [
                jnp.concatenate([coarse[base + 2 * i + j] for j in range(4)], axis=1)
                for i in range(fold)
            ],
            axis=0,
        )
        y = across_taps(matmul(lhs, wide1[...]), 2 * HEAD, cols)
        for i in range(fold):
            field5[base + 2 * i] = y[i * cols : (i + 1) * cols, :HEAD]
            field5[base + 2 * i + 1] = y[i * cols : (i + 1) * cols, HEAD:]
        total, square = sums(y)
        stats5[q, 0:1] = total
        stats5[q, 1:2] = square
        return carry

    lax.fori_loop(0, lines // (2 * fold), step, 0, unroll=True)
    wait_y2.wait()
    norm2 = merged_norm([(b[0:1], b[1:2]) for b in blocks], y2.shape[1] * (y2.shape[0] - 4), 2)
    acts = [normed(y2[i], *norm2) for i in range(y2.shape[0])]
    count = len(acts)
    acts[1] = jnp.where(first, acts[2], acts[1])
    acts[count - 2] = jnp.where(last, acts[count - 3], acts[count - 2])
    merged4 = up_conv(acts, wide0, c4, c4_out, stats4)
    out += outer.work()
    parts5 = []
    for q in range(lines // (2 * fold)):
        parts5 += halves((stats5[q, 0:1], stats5[q, 1:2]))
    norm5 = merged_norm(parts5, cols * fold, 5)
    band = lines // members
    acts = []
    for i in range(band + 4):
        at = jnp.clip(position * band + (i - 2), 0, lines - 1)
        acts.append(normed(field5[at], *norm5))
    merged6 = up_conv(acts, wide2, c6, c6_out, stats6)
    parts0, parts1 = [], []
    for stats in (inner0, outer0):
        for p in range(stats.shape[0]):
            parts0 += halves((stats[p, 0:1], stats[p, 1:2]))
    for p in range(inner1.shape[0]):
        parts1 += halves((inner1[p, 0:1], inner1[p, 1:2]))
    for p in range(2):
        parts1.append(halves((outer1[p, 0:1], outer1[p, 1:2]))[1 - p])
    eighth_cols = c4.shape[1]
    merged = [merge(parts0, 2 * eighth_cols), merge(parts1, eighth_cols), merged4, merged6]
    pad = [jnp.zeros((4, HEAD), F32)]
    block = jnp.concatenate([m[0] for m in merged] + pad + [m[1] for m in merged] + pad, axis=0)
    for i in range(members):
        pieces[i] = block
    for copy in out:
        copy.wait()


def final_kernel(
    place, bias, got, gain, shift, inner0, outer0, inner1, outer1, stats4, stats6, labels, class_t, class_t3, up_cols,
    c0_in, c1_in, c4_in, c6_in, logits, pieces, c0, c1, c4, c6, lines, doubled, scores, sems,
):
    members = got.shape[0]
    copies = Copies(sems)
    waits = [copies.start(a, b) for a, b in ((c1_in, c1), (c4_in, c4), (c6_in, c6))]
    rows = c0.shape[0]
    wait0 = copies.start(c0_in, c0)
    count = c4.shape[0]
    first, last = place[0] == 0, place[0] == members - 1
    row = lax.broadcasted_iota(jnp.int32, (8, HEAD), 0)
    own = float((count - 2) * c4.shape[1])
    pixels = jnp.where(row == 0, 4.0 * own, own)
    total = sum(got[i, 0:8] for i in range(members))
    mean = group_sum(total) / (pixels * (members * GROUP))
    square = sum(got[i, 8:16] + pixels * jnp.square(got[i, 0:8] / pixels - mean) for i in range(members))
    scale = lax.rsqrt(group_sum(square) / (pixels * (members * GROUP)) + NORM_FLOOR)
    norms = [
        (mean[j : j + 1], gain[layer : layer + 1] * scale[j : j + 1], shift[layer : layer + 1])
        for j, layer in enumerate((0, 1, 4, 6))
    ]

    def lift(field, r, total, norm):
        half = total[:, (r % 2) * HEAD : (r % 2 + 1) * HEAD]
        return lifted(field[r], norm[1], offset(half, field.shape[1], norm))

    def joined(inner, outer):
        pairs = [inner[p, 0:1] for p in range(inner.shape[0])]
        return [outer[0, 0:1]] + pairs + [outer[1, 0:1]]

    totals0, totals1 = joined(inner0, outer0), joined(inner1, outer1)
    for wait in waits:
        wait.wait()
    for i in range(count):
        p = i // 2
        acts = [
            lift(c1, i, totals1[p], norms[1]),
            lift(c4, i, stats4[p, 0:1], norms[2]),
            lift(c6, i, stats6[p, 0:1], norms[3]),
        ]
        lines[i] = matmul_t(class_t3[...], jnp.concatenate(acts, axis=1))
    lines[0] = jnp.where(first, lines[1], lines[0])
    lines[count - 1] = jnp.where(last, lines[count - 2], lines[count - 1])
    for i in range(count):
        value = lines[i]
        high = value.astype(BF16)
        low = (value - high.astype(F32)).astype(BF16)
        both = matmul(jnp.concatenate([high, low], axis=0), up_cols[...])
        doubled[i] = both[:SLOT] + both[SLOT:]
    wait0.wait()
    for r in range(rows):
        p = r // 2
        value = matmul_t(class_t[...], lift(c0, r, totals0[p], norms[0]))
        value = value + (0.75 * doubled[p + 1] + 0.25 * doubled[p + 2 * (r % 2)])
        for i in range(scores.shape[0]):
            scores[i, r * SLOT : (r + 1) * SLOT] = value[:, i * HEAD : (i + 1) * HEAD]
    label_map = labels[...]
    exps = jnp.zeros(label_map.shape, F32)
    picked = jnp.zeros(label_map.shape, F32)
    for c in range(logits.shape[0]):
        tiles = [scores.at[i][pl.ds(c, rows, stride=SLOT), :] for i in range(scores.shape[0])]
        score = jnp.concatenate(tiles, axis=1) + bias[c]
        logits[c] = score.astype(BF16)
        exps = exps + jnp.exp(score)
        picked = picked + jnp.where(label_map == c, score, 0.0)
    usable = label_map != 255
    terms = jnp.where(usable, jnp.log(exps) - picked, 0.0)
    counts = jnp.where(usable, 1.0, 0.0)
    out = []
    for v in (terms, counts):
        v = jnp.sum(v, axis=0, keepdims=True)
        out.append(sum(v[:, i * HEAD : (i + 1) * HEAD] for i in range(v.shape[1] // HEAD)))
    both = jnp.concatenate(out, axis=0)
    for i in range(pieces.shape[0]):
        pieces[i] = both


def params_of(**kw):
    return pltpu.CompilerParams(vmem_limit_bytes=VMEM_LIMIT, **kw)


def shaped(shape, dtype):
    return jax.ShapeDtypeStruct(shape, dtype)


VM = pl.BlockSpec(memory_space=pltpu.VMEM)
SM = pl.BlockSpec(memory_space=pltpu.SMEM)
ANY = pl.BlockSpec(memory_space=pl.ANY)


def device_step(
    feat_quarter,
    feat_eighth,
    feat_sixteenth,
    feat_thirty,
    labels,
    first_weights,
    inner_weights,
    norm_gain,
    norm_shift,
    class_weight,
    class_bias,
):
    position = lax.axis_index(ROWS)
    bands = lax.axis_size(ROWS)
    devices = bands * lax.axis_size(BATCH)
    place = position.astype(jnp.int32).reshape(1)
    up_pairs = [(i, i + 1) for i in range(bands - 1)]
    down_pairs = [(j, i) for i, j in up_pairs]
    feats = [feat_quarter[0], feat_eighth[0], feat_sixteenth[0], feat_thirty[0]]
    quarter, eighth, sixteenth, thirty = feats
    q_rows, q_cols, depth = quarter.shape
    e_rows, e_cols, _ = eighth.shape
    s_rows, s_cols, _ = sixteenth.shape
    t_rows, t_cols, _ = thirty.shape
    small = shaped((SMALL[0] * s_cols + SMALL[1] * t_cols, depth), BF16)
    big = shaped((BIG[0] * q_cols + BIG[1] * e_cols, depth), BF16)
    small_before, small_after, big_before, big_after = pl.pallas_call(
        edges_kernel,
        out_shape=[small, small, big, big],
        in_specs=[ANY] * 4,
        out_specs=[VM] * 4,
        scratch_shapes=[pltpu.SemaphoreType.DMA((2 * (sum(SMALL) + sum(BIG)),))],
        compiler_params=params_of(),
        name="edges",
    )(*feats)
    small_before = lax.ppermute(small_before, ROWS, up_pairs)
    small_after = lax.ppermute(small_after, ROWS, down_pairs)
    big_before = lax.ppermute(big_before, ROWS, up_pairs)
    big_after = lax.ppermute(big_after, ROWS, down_pairs)

    def fixed(a, *index):
        index = index or (0,) * len(a.shape)
        return pl.BlockSpec(a.shape, lambda i: index)

    def weight(level):
        return pl.BlockSpec((None,) + first_weights.shape[1:], lambda i: (level, 0, 0, 0, 0))

    deep = pltpu.VMEM((4 * depth, 4 * HEAD), BF16)
    raw = pltpu.VMEM(first_weights.shape[1:], BF16)
    pairs = q_rows // 2
    steps = e_rows // 2 + 1
    field0 = shaped((q_rows, q_cols, HEAD), BF16)
    field1 = shaped((e_rows + 2, e_cols, HEAD), BF16)
    stats_shape = lambda n: shaped((n, 8, 2 * HEAD), F32)
    room = lambda a: pltpu.VMEM(a.shape, a.dtype)
    piece = shaped((bands, STAT_ROWS + t_rows * t_cols, HEAD), BF16)
    y2_shape = shaped((s_rows + 4, s_cols, HEAD), F32)
    coarse_call = pl.pallas_call(
        coarse_kernel,
        grid=(1,),
        out_shape=[y2_shape, piece],
        in_specs=[fixed(small), fixed(small), fixed(sixteenth), fixed(thirty), weight(2), weight(3)],
        out_specs=[fixed(y2_shape), fixed(piece)],
        scratch_shapes=[deep, deep],
        compiler_params=pltpu.CompilerParams(vmem_limit_bytes=20*1024*1024),
        name="coarse",
    )
    y2, pieces = coarse_call(
        small_before, small_after, sixteenth, thirty, first_weights, first_weights
    )
    got = everyone(pieces, ROWS)
    inside0, inside1 = pairs - 2, steps - 2
    c0, c1, inner0, inner1 = pl.pallas_call(
        inner_kernel,
        out_shape=[field0, field1, stats_shape(inside0), stats_shape(inside1)],
        in_specs=[ANY] * 4,
        out_specs=[ANY, ANY, VM, VM],
        scratch_shapes=[
            room(quarter), room(eighth), raw, raw, deep, deep, room(field0), room(field1),
            pltpu.SemaphoreType.DMA((2 * inside0 + inside1 + 3,)),
        ],
        compiler_params=params_of(),
        name="inner",
    )(quarter, eighth, first_weights, y2)
    up_small = jnp.asarray(doubling(t_cols), BF16)
    up_big = jnp.asarray(doubling(s_cols), BF16)
    up_cols = jnp.asarray(doubling(e_cols).T, BF16)
    narrow = pltpu.VMEM((4 * HEAD, 6 * HEAD), BF16)
    c0, c1, outer0, outer1, c4, c6, stats4, stats6, pieces = pl.pallas_call(
        between_kernel,
        out_shape=[
            field0, field1, stats_shape(2), stats_shape(2),
            field1, field1, stats_shape(steps), stats_shape(steps), shaped((bands, 16, HEAD), F32),
        ],
        in_specs=[SM, VM, ANY, ANY] + [VM] * 6 + [ANY] * 7,
        out_specs=[ANY, ANY, VM, VM, ANY, ANY, VM, VM, VM],
        input_output_aliases={15: 0, 16: 1},
        scratch_shapes=[
            room(y2), room(inner_weights), room(field1), room(field1),
            pltpu.VMEM((e_rows + 4, e_cols, HEAD), BF16),
            pltpu.VMEM((2 * t_rows * bands + 2, 2 * t_cols, HEAD), BF16),
            pltpu.VMEM((2 * t_rows * bands, 2 * t_cols, HEAD), F32),
            pltpu.VMEM((t_rows * bands, 8, 2 * HEAD), F32),
            narrow, narrow, narrow,
            pltpu.SemaphoreType.DMA((2 * steps + 14,)),
            pltpu.VMEM((6, q_cols, depth), BF16), pltpu.VMEM((4, e_cols, depth), BF16), room(big), room(big),
            raw, raw, deep, deep,
            pltpu.VMEM((4, q_cols, HEAD), BF16), pltpu.VMEM((4, e_cols, HEAD), BF16),
        ],
        compiler_params=params_of(),
        name="between",
    )(
        place, got, y2, inner_weights, norm_gain, norm_shift, up_small, up_big,
        inner0, inner1, quarter, eighth, big_before, big_after, first_weights, c0, c1,
    )
    got = everyone(pieces, ROWS)
    classes = class_weight.shape[1]
    class_t = jnp.pad(class_weight.T, ((0, SLOT - classes), (0, 0)))
    class_t3 = jnp.concatenate([class_t] * 3, axis=1)
    logits, pieces = pl.pallas_call(
        final_kernel,
        out_shape=[shaped((classes, q_rows, q_cols), BF16), shaped((devices, 2, HEAD), F32)],
        in_specs=[SM, SM] + [VM] * 13 + [ANY] * 4,
        out_specs=[VM, VM],
        scratch_shapes=[
            room(field0), room(field1), room(field1), room(field1),
            pltpu.VMEM((e_rows + 2, SLOT, e_cols), F32),
            pltpu.VMEM((e_rows + 2, SLOT, q_cols), F32),
            pltpu.VMEM((q_cols // HEAD, q_rows * SLOT, HEAD), F32),
            pltpu.SemaphoreType.DMA((7,)),
        ],
        compiler_params=params_of(),
        name="final",
    )(
        place, class_bias, got, norm_gain, norm_shift, inner0, outer0, inner1, outer1, stats4, stats6,
        labels[0], class_t, class_t3, up_cols, c0, c1, c4, c6,
    )
    loss_total, valid_count = jnp.sum(everyone(pieces, EVERY), axis=(0, 2))
    mean_loss = loss_total / jnp.maximum(valid_count, 1.0)
    return (logits[None], mean_loss)


def solution(mesh):
    split = Mesh(mesh.devices.reshape(4, 2, 4, 4), ("batch_0", "batch_1", "rows_0", "rows_1"))
    in_specs = (
        P(BATCH, ROWS, None, None),
        P(BATCH, ROWS, None, None),
        P(BATCH, ROWS, None, None),
        P(BATCH, ROWS, None, None),
        P(BATCH, ROWS, None),
        P(),
        P(),
        P(),
        P(),
        P(),
        P(),
    )
    out_specs = (P(BATCH, None, ROWS, None), P())
    return jax.shard_map(device_step, mesh=split, in_specs=in_specs, out_specs=out_specs, check_vma=False)
```

```python
import jax
import jax.numpy as jnp
import numpy as np
from jax import lax
from jax.experimental import pallas as pl
from jax.experimental.pallas import tpu as pltpu
from jax.sharding import Mesh
from jax.sharding import PartitionSpec as P

GROUP = 4
HEAD = 128
ROWS = ("rows_0", "rows_1")
EVERY = ("batch_0", "batch_1", "rows_0", "rows_1")
BATCH = ("batch_0", "batch_1")
NORM_FLOOR = 0.05
SMALL = (3, 1)
BIG = (1, 2)
STAT_ROWS = 16
SLOT = 32
F32, BF16 = jnp.float32, jnp.bfloat16
VMEM_LIMIT = 60 * 1024 * 1024


def doubling(cols):
    matrix = np.zeros((2 * cols, cols), np.float32)
    for k in range(cols):
        matrix[2 * k, k] += 0.75
        matrix[2 * k, max(k - 1, 0)] += 0.25
        matrix[2 * k + 1, k] += 0.75
        matrix[2 * k + 1, min(k + 1, cols - 1)] += 0.25
    return matrix


def everyone(pieces, axes):
    return lax.all_to_all(pieces, axes, 0, 0)


def matmul(a, b):
    return jnp.dot(a, b, preferred_element_type=F32)


def matmul_t(a, b):
    return lax.dot_general(a, b, (((1,), (1,)), ((), ())), preferred_element_type=F32)


def fill_pair(w_ref, out_ref, depth):
    zero = jnp.zeros((depth, HEAD), BF16)
    for j in range(4):
        for across in range(3):
            rows = slice(j * depth, (j + 1) * depth)
            at = across * 2 * HEAD
            out_ref[rows, at : at + HEAD] = w_ref[j, across] if j < 3 else zero
            out_ref[rows, at + HEAD : at + 2 * HEAD] = w_ref[j - 1, across] if j else zero


def across_taps(z, width, cols):
    pixels = z.shape[0]
    index = lax.broadcasted_iota(jnp.int32, (pixels, width), 0) % cols
    left = jnp.where(index == 0, 0.0, pltpu.roll(z[:, :width], 1, 0))
    right = jnp.where(index == cols - 1, 0.0, pltpu.roll(z[:, 2 * width :], pixels - 1, 0))
    return z[:, width : 2 * width] + left + right


def conv_pair(rows, w_ref):
    return across_taps(matmul(jnp.concatenate(rows, axis=1), w_ref[...]), 2 * HEAD, rows[0].shape[0])


def fill_deep(w_ref, out_ref, depth):
    zero = jnp.zeros((depth, HEAD), BF16)
    for j in range(4):
        rows = slice(j * depth, (j + 1) * depth)
        if j < 3:
            out_ref[rows, :HEAD] = w_ref[j, 0]
            out_ref[rows, HEAD : 2 * HEAD] = w_ref[j, 1]
        out_ref[rows, 2 * HEAD : 3 * HEAD] = w_ref[j, 2] if j < 3 else zero
        out_ref[rows, 3 * HEAD :] = w_ref[j - 1, 2] if j else zero


def conv_deep(rows, w_ref):
    cols, depth = rows[0].shape
    wide = jnp.concatenate(rows, axis=1)
    stacked = jnp.concatenate([wide[:, : 3 * depth], wide[:, depth:]], axis=0)
    near = matmul(stacked, w_ref[: 3 * depth, : 2 * HEAD])
    far = matmul(wide, w_ref[:, 2 * HEAD :])
    taps = [jnp.concatenate([near[:cols, at : at + HEAD], near[cols:, at : at + HEAD]], axis=1) for at in (0, HEAD)]
    index = lax.broadcasted_iota(jnp.int32, far.shape, 0)
    left = jnp.where(index == 0, 0.0, pltpu.roll(taps[0], 1, 0))
    right = jnp.where(index == cols - 1, 0.0, pltpu.roll(far, cols - 1, 0))
    return taps[1] + left + right


def centre(y):
    total = jnp.sum(y, axis=0, keepdims=True)
    centred = y - total * (1.0 / y.shape[0])
    return total, jnp.sum(centred * centred, axis=0, keepdims=True), centred


def sums(y):
    return centre(y)[:2]


def merge(parts, pixels):
    total = sum(p[0] for p in parts)
    mean = total * (1.0 / (pixels * len(parts)))
    square = sum(p[1] + pixels * jnp.square(p[0] * (1.0 / pixels) - mean) for p in parts)
    return total, square


def halves(pair):
    total, square = pair
    return [(total[:, :HEAD], square[:, :HEAD]), (total[:, HEAD:], square[:, HEAD:])]


def group_sum(v):
    lane = lax.broadcasted_iota(jnp.int32, v.shape, 1)
    v = v + jnp.where(lane % 2 == 0, pltpu.roll(v, HEAD - 1, 1), pltpu.roll(v, 1, 1))
    return v + jnp.where(lane % 4 < 2, pltpu.roll(v, HEAD - 2, 1), pltpu.roll(v, 2, 1))


def normed(y, mean, factor, shift):
    return jnp.maximum((y - mean) * factor + shift, 0.0).astype(BF16)


def offset(total, pixels, norm):
    mean, factor, shift = norm
    return (total * (1.0 / pixels) - mean) * factor + shift


def lifted(centred, factor, at):
    return jnp.maximum(centred.astype(F32) * factor + at, 0.0).astype(BF16)


def split_rows(values):
    high = values.astype(BF16).astype(F32)
    rest = values - high
    middle = rest.astype(BF16).astype(F32)
    return [high, middle, rest - middle]


def edges_kernel(quarter, eighth, sixteenth, thirty, small_before, small_after, big_before, big_after, sems):
    copies = []
    groups = (
        (SMALL, (sixteenth, thirty), small_before, small_after),
        (BIG, (quarter, eighth), big_before, big_after),
    )
    for depths, feats, before, after in groups:
        at = 0
        for depth, feat in zip(depths, feats):
            rows, cols, _ = feat.shape
            for i in range(depth):
                spot = pl.ds(at, cols)
                copies.append((feat.at[rows - depth + i], before.at[spot]))
                copies.append((feat.at[i], after.at[spot]))
                at += cols
    started = [pltpu.make_async_copy(a, b, sems.at[i]) for i, (a, b) in enumerate(copies)]
    for copy in started:
        copy.start()
    for copy in started:
        copy.wait()


class Copies:
    def __init__(self, sems):
        self.sems, self.used = sems, 0

    def start(self, source, target):
        copy = pltpu.make_async_copy(source, target, self.sems.at[self.used])
        self.used += 1
        copy.start()
        return copy


def keep_pair(y, field, stats, index, pair):
    total, square, centred = centre(y)
    field[2 * pair] = centred[:, :HEAD].astype(BF16)
    field[2 * pair + 1] = centred[:, HEAD:].astype(BF16)
    stats[index, 0:1] = total
    stats[index, 1:2] = square


def inner_kernel(
    quarter, eighth, weights, _, c0_out, c1_out, stats0, stats1, x0, x1, w0, w1, deep0, deep1, c0, c1, sems
):
    copies = Copies(sems)
    rows0 = pl.ds(1, quarter.shape[0] - 2)
    waits1 = [copies.start(weights.at[1], w1), copies.start(eighth, x1)]
    waits0 = [copies.start(weights.at[0], w0), copies.start(quarter.at[rows0], x0.at[rows0])]
    out = []
    for wait in waits1:
        wait.wait()
    fill_deep(w1, deep1, 2 * HEAD)
    for i in range(stats1.shape[0]):
        p = i + 1
        keep_pair(conv_deep([x1[2 * i + j] for j in range(4)], deep1), c1, stats1, i, p)
        out.append(copies.start(c1.at[pl.ds(2 * p, 2)], c1_out.at[pl.ds(2 * p, 2)]))
    for wait in waits0:
        wait.wait()
    fill_deep(w0, deep0, 2 * HEAD)
    for i in range(stats0.shape[0]):
        p = i + 1
        keep_pair(conv_deep([x0[2 * i + 1 + j] for j in range(4)], deep0), c0, stats0, i, p)
        out.append(copies.start(c0.at[pl.ds(2 * p, 2)], c0_out.at[pl.ds(2 * p, 2)]))
    for copy in out:
        copy.wait()


class Outer:
    def __init__(self, copies, inputs, outputs, room):
        self.copies, self.outputs, self.room = copies, outputs, room
        quarter, eighth, before, after, weights = inputs
        x0, x1, low, high, w0, w1 = room[:6]
        self.q_rows, self.cols, _ = quarter.shape
        self.e_rows, self.e_cols, _ = eighth.shape
        pairs = (
            (weights.at[1], w1),
            (weights.at[0], w0),
            (before, low),
            (after, high),
            (eighth.at[pl.ds(0, 2)], x1.at[pl.ds(0, 2)]),
            (eighth.at[pl.ds(self.e_rows - 2, 2)], x1.at[pl.ds(2, 2)]),
            (quarter.at[pl.ds(0, 3)], x0.at[pl.ds(0, 3)]),
            (quarter.at[pl.ds(self.q_rows - 3, 3)], x0.at[pl.ds(3, 3)]),
        )
        self.waits = [copies.start(*pair) for pair in pairs]

    def work(self):
        for wait in self.waits:
            wait.wait()
        c0_out, c1_out, stats0, stats1 = self.outputs
        x0, x1, low, high, w0, w1, deep0, deep1, c0, c1 = self.room
        fill_deep(w1, deep1, 2 * HEAD)
        fill_deep(w0, deep0, 2 * HEAD)
        cols, e_cols = self.cols, self.e_cols
        for i in range(2):
            rows = [x0[3 * i + j] for j in range(3)]
            keep_pair(conv_deep(rows + [high[:cols]] if i else [low[:cols]] + rows, deep0), c0, stats0, i, i)
        for i in range(2):
            halo = high if i else low
            rows = [x1[2 * i + j] for j in range(2)]
            extra = [halo[cols + j * e_cols : cols + (j + 1) * e_cols] for j in range(2)]
            keep_pair(conv_deep(rows + extra if i else extra + rows, deep1), c1, stats1, i, i)
        out = []
        for i in range(2):
            spot = pl.ds(2 * i, 2)
            out.append(self.copies.start(c0.at[spot], c0_out.at[pl.ds(i * (self.q_rows - 2), 2)]))
            out.append(self.copies.start(c1.at[spot], c1_out.at[pl.ds(i * self.e_rows, 2)]))
        return out


def coarse_kernel(before, after, sixteenth, thirty, w2, w3, y2, pieces, wide2, wide3):
    depth = 2 * HEAD
    fill_deep(w2, wide2, depth)
    fill_deep(w3, wide3, depth)
    own, cols, _ = sixteenth.shape
    ring = SMALL[0]
    rows = [before[i * cols : (i + 1) * cols] for i in range(ring)]
    rows += [sixteenth[i] for i in range(own)]
    rows += [after[i * cols : (i + 1) * cols] for i in range(ring)]
    parts = []
    for p in range(y2.shape[0] // 2):
        out = conv_deep(rows[2 * p : 2 * p + 4], wide2)
        y2[2 * p] = out[:, :HEAD]
        y2[2 * p + 1] = out[:, HEAD:]
        if 0 < p < y2.shape[0] // 2 - 1:
            parts += halves(sums(out))
    at = ring * cols
    out = conv_deep([before[at:], thirty[0], thirty[1], after[at:]], wide3)
    total3, square3, coarse = centre(jnp.concatenate([out[:, :HEAD], out[:, HEAD:]], axis=0))
    coarse = coarse.astype(BF16)
    total, square = merge(parts, cols)
    values = jnp.concatenate([total, square, total3, square3], axis=0)
    head = jnp.concatenate(split_rows(values) + [jnp.zeros((4, HEAD), F32)], axis=0).astype(BF16)
    for i in range(pieces.shape[0]):
        pieces[i, :STAT_ROWS] = head
        pieces[i, STAT_ROWS:] = coarse


def between_kernel(
    place, got, y2_in, weights_in, gain, shift, up_small, up_big, inner0, inner1,
    quarter, eighth, before, after, first_weights, _, __,
    c0_out, c1_out, outer0, outer1, c4_out, c6_out, stats4, stats6, pieces,
    y2, weights, c4, c6, fine, coarse, field5, stats5, wide0, wide1, wide2, sems, *room,
):
    members = got.shape[0]
    position = place[0]
    first, last = position == 0, position == members - 1
    copies = Copies(sems)
    wait_w = copies.start(weights_in, weights)
    wait_y2 = copies.start(y2_in, y2)
    outer = Outer(
        copies, (quarter, eighth, before, after, first_weights), (c0_out, c1_out, outer0, outer1), room
    )
    out = []

    def merged_norm(each, pixels, layer):
        count = pixels * len(each) * GROUP
        mean = group_sum(jnp.broadcast_to(sum(p[0] for p in each), (8, HEAD)))[0:1] * (1.0 / count)
        square = sum(p[1] + pixels * jnp.square(p[0] * (1.0 / pixels) - mean) for p in each)
        var = group_sum(jnp.broadcast_to(square, (8, HEAD)))[0:1] * (1.0 / count)
        return mean, gain[layer : layer + 1] * lax.rsqrt(var + NORM_FLOOR), shift[layer : layer + 1]

    def up_conv(acts, wide, kept, kept_out, stats):
        count = len(acts)
        doubled = []
        for k in range(0, count, 2):
            both = matmul(up_big[...], jnp.concatenate([acts[k], acts[k + 1]], axis=1))
            doubled += [both[:, :HEAD], both[:, HEAD:]]
        lines = 2 * (count - 2)
        for k in range(1, count - 1):
            for half, other in ((0, k - 1), (1, k + 1)):
                line = 0.75 * doubled[k] + 0.25 * doubled[other]
                at = 2 * (k - 1) + half
                if at < 2:
                    line = jnp.where(first, 0.0, line)
                if at >= lines - 2:
                    line = jnp.where(last, 0.0, line)
                fine[at] = line.astype(BF16)
        own = []
        for p in range(lines // 2 - 1):
            keep_pair(conv_pair([fine[2 * p + j] for j in range(4)], wide), kept, stats, p, p)
            span = pl.ds(2 * p, 2)
            out.append(copies.start(kept.at[span], kept_out.at[span]))
            two = halves((stats[p, 0:1], stats[p, 1:2]))
            own += two[1:] if p == 0 else two[:1] if p == lines // 2 - 2 else two
        return merge(own, kept.shape[1])

    lines, cols = coarse.shape[0] - 2, coarse.shape[1]
    small = cols // 2
    blocks = [got[i, :STAT_ROWS].astype(F32) for i in range(members)]
    blocks = [b[0:4] + b[4:8] + b[8:12] for b in blocks]
    norm3 = merged_norm([(b[2:3], b[3:4]) for b in blocks], 2 * small, 3)
    doubled = []
    for i in range(members):
        a = lifted(got[i, STAT_ROWS:], norm3[1], offset(blocks[i][2:3], 2 * small, norm3))
        both = matmul(up_small[...], jnp.concatenate([a[:small], a[small:]], axis=1))
        doubled += [both[:, :HEAD], both[:, HEAD:]]
    coarse[0] = jnp.zeros((cols, HEAD), BF16)
    coarse[lines + 1] = jnp.zeros((cols, HEAD), BF16)
    for k in range(len(doubled)):
        for half, other in ((0, max(k - 1, 0)), (1, min(k + 1, len(doubled) - 1))):
            coarse[1 + 2 * k + half] = (0.75 * doubled[k] + 0.25 * doubled[other]).astype(BF16)
    wait_w.wait()
    for i, wide in enumerate((wide0, wide1, wide2)):
        fill_pair(weights.at[i], wide, HEAD)
    fold = 4

    def step(q, carry):
        base = q * (2 * fold)
        lhs = jnp.concatenate(
            [
                jnp.concatenate([coarse[base + 2 * i + j] for j in range(4)], axis=1)
                for i in range(fold)
            ],
            axis=0,
        )
        y = across_taps(matmul(lhs, wide1[...]), 2 * HEAD, cols)
        for i in range(fold):
            field5[base + 2 * i] = y[i * cols : (i + 1) * cols, :HEAD]
            field5[base + 2 * i + 1] = y[i * cols : (i + 1) * cols, HEAD:]
        total, square = sums(y)
        stats5[q, 0:1] = total
        stats5[q, 1:2] = square
        return carry

    lax.fori_loop(0, lines // (2 * fold), step, 0, unroll=True)
    out += outer.work()
    wait_y2.wait()
    norm2 = merged_norm([(b[0:1], b[1:2]) for b in blocks], y2.shape[1] * (y2.shape[0] - 4), 2)
    acts = [normed(y2[i], *norm2) for i in range(y2.shape[0])]
    count = len(acts)
    acts[1] = jnp.where(first, acts[2], acts[1])
    acts[count - 2] = jnp.where(last, acts[count - 3], acts[count - 2])
    merged4 = up_conv(acts, wide0, c4, c4_out, stats4)
    parts5 = []
    for q in range(lines // (2 * fold)):
        parts5 += halves((stats5[q, 0:1], stats5[q, 1:2]))
    norm5 = merged_norm(parts5, cols * fold, 5)
    band = lines // members
    acts = []
    for i in range(band + 4):
        at = jnp.clip(position * band + (i - 2), 0, lines - 1)
        acts.append(normed(field5[at], *norm5))
    merged6 = up_conv(acts, wide2, c6, c6_out, stats6)
    parts0, parts1 = [], []
    for stats in (inner0, outer0):
        for p in range(stats.shape[0]):
            parts0 += halves((stats[p, 0:1], stats[p, 1:2]))
    for p in range(inner1.shape[0]):
        parts1 += halves((inner1[p, 0:1], inner1[p, 1:2]))
    for p in range(2):
        parts1.append(halves((outer1[p, 0:1], outer1[p, 1:2]))[1 - p])
    eighth_cols = c4.shape[1]
    merged = [merge(parts0, 2 * eighth_cols), merge(parts1, eighth_cols), merged4, merged6]
    block = jnp.concatenate([m[0] for m in merged] + [m[1] for m in merged], axis=0)
    for i in range(members):
        pieces[i] = block
    for copy in out:
        copy.wait()


def final_kernel(
    place, bias, got, gain, shift, inner0, outer0, inner1, outer1, stats4, stats6, labels, class_t, class_t3, up_cols,
    c1, c4, c6, c0_in, logits, pieces, c0, lines, doubled, scores, sems,
):
    members = got.shape[0]
    copies = Copies(sems)
    rows = c0.shape[0]
    wait0 = copies.start(c0_in, c0)
    count = c4.shape[0]
    first, last = place[0] == 0, place[0] == members - 1
    row = lax.broadcasted_iota(jnp.int32, (4, HEAD), 0)
    own = float((count - 2) * c4.shape[1])
    pixels = jnp.where(row == 0, 4.0 * own, own)
    total = sum(got[i, 0:4] for i in range(members))
    mean = group_sum(total) / (pixels * (members * GROUP))
    square = sum(got[i, 4:8] + pixels * jnp.square(got[i, 0:4] / pixels - mean) for i in range(members))
    scale = lax.rsqrt(group_sum(square) / (pixels * (members * GROUP)) + NORM_FLOOR)
    norms = [
        (mean[j : j + 1], gain[layer : layer + 1] * scale[j : j + 1], shift[layer : layer + 1])
        for j, layer in enumerate((0, 1, 4, 6))
    ]

    def lift(field, r, total, norm):
        half = total[:, (r % 2) * HEAD : (r % 2 + 1) * HEAD]
        return lifted(field[r], norm[1], offset(half, field.shape[1], norm))

    def joined(inner, outer):
        pairs = [inner[p, 0:1] for p in range(inner.shape[0])]
        return [outer[0, 0:1]] + pairs + [outer[1, 0:1]]

    totals0, totals1 = joined(inner0, outer0), joined(inner1, outer1)
    for i in range(count):
        p = i // 2
        acts = [
            lift(c1, i, totals1[p], norms[1]),
            lift(c4, i, stats4[p, 0:1], norms[2]),
            lift(c6, i, stats6[p, 0:1], norms[3]),
        ]
        lines[i] = matmul_t(class_t3[...], jnp.concatenate(acts, axis=1))
    lines[0] = jnp.where(first, lines[1], lines[0])
    lines[count - 1] = jnp.where(last, lines[count - 2], lines[count - 1])
    for i in range(count):
        value = lines[i]
        high = value.astype(BF16)
        low = (value - high.astype(F32)).astype(BF16)
        both = matmul(jnp.concatenate([high, low], axis=0), up_cols[...])
        doubled[i] = both[:SLOT] + both[SLOT:]
    wait0.wait()
    for r in range(rows):
        p = r // 2
        value = matmul_t(class_t[...], lift(c0, r, totals0[p], norms[0]))
        value = value + (0.75 * doubled[p + 1] + 0.25 * doubled[p + 2 * (r % 2)])
        for i in range(scores.shape[0]):
            scores[i, r * SLOT : (r + 1) * SLOT] = value[:, i * HEAD : (i + 1) * HEAD]
    label_map = labels[...]
    exps = jnp.zeros(label_map.shape, F32)
    picked = jnp.zeros(label_map.shape, F32)
    for c in range(logits.shape[0]):
        tiles = [scores.at[i][pl.ds(c, rows, stride=SLOT), :] for i in range(scores.shape[0])]
        score = jnp.concatenate(tiles, axis=1) + bias[c]
        logits[c] = score.astype(BF16)
        exps = exps + jnp.exp(score)
        picked = picked + jnp.where(label_map == c, score, 0.0)
    usable = label_map != 255
    terms = jnp.where(usable, jnp.log(exps) - picked, 0.0)
    counts = jnp.where(usable, 1.0, 0.0)
    out = []
    for v in (terms, counts):
        v = jnp.sum(v, axis=0, keepdims=True)
        out.append(sum(v[:, i * HEAD : (i + 1) * HEAD] for i in range(v.shape[1] // HEAD)))
    both = jnp.concatenate(out, axis=0)
    for i in range(pieces.shape[0]):
        pieces[i] = both


def params_of(**kw):
    return pltpu.CompilerParams(vmem_limit_bytes=VMEM_LIMIT, **kw)


def shaped(shape, dtype):
    return jax.ShapeDtypeStruct(shape, dtype)


VM = pl.BlockSpec(memory_space=pltpu.VMEM)
SM = pl.BlockSpec(memory_space=pltpu.SMEM)
ANY = pl.BlockSpec(memory_space=pl.ANY)


def device_step(
    feat_quarter,
    feat_eighth,
    feat_sixteenth,
    feat_thirty,
    labels,
    first_weights,
    inner_weights,
    norm_gain,
    norm_shift,
    class_weight,
    class_bias,
):
    position = lax.axis_index(ROWS)
    bands = lax.axis_size(ROWS)
    devices = bands * lax.axis_size(BATCH)
    place = position.astype(jnp.int32).reshape(1)
    up_pairs = [(i, i + 1) for i in range(bands - 1)]
    down_pairs = [(j, i) for i, j in up_pairs]
    feats = [feat_quarter[0], feat_eighth[0], feat_sixteenth[0], feat_thirty[0]]
    quarter, eighth, sixteenth, thirty = feats
    q_rows, q_cols, depth = quarter.shape
    e_rows, e_cols, _ = eighth.shape
    s_rows, s_cols, _ = sixteenth.shape
    t_rows, t_cols, _ = thirty.shape
    small = shaped((SMALL[0] * s_cols + SMALL[1] * t_cols, depth), BF16)
    big = shaped((BIG[0] * q_cols + BIG[1] * e_cols, depth), BF16)
    small_before, small_after, big_before, big_after = pl.pallas_call(
        edges_kernel,
        out_shape=[small, small, big, big],
        in_specs=[ANY] * 4,
        out_specs=[VM] * 4,
        scratch_shapes=[pltpu.SemaphoreType.DMA((2 * (sum(SMALL) + sum(BIG)),))],
        compiler_params=params_of(),
        name="edges",
    )(*feats)
    small_before = lax.ppermute(small_before, ROWS, up_pairs)
    small_after = lax.ppermute(small_after, ROWS, down_pairs)
    big_before = lax.ppermute(big_before, ROWS, up_pairs)
    big_after = lax.ppermute(big_after, ROWS, down_pairs)

    def fixed(a, *index):
        index = index or (0,) * len(a.shape)
        return pl.BlockSpec(a.shape, lambda i: index)

    def weight(level):
        return pl.BlockSpec((None,) + first_weights.shape[1:], lambda i: (level, 0, 0, 0, 0))

    deep = pltpu.VMEM((4 * depth, 4 * HEAD), BF16)
    raw = pltpu.VMEM(first_weights.shape[1:], BF16)
    pairs = q_rows // 2
    steps = e_rows // 2 + 1
    field0 = shaped((q_rows, q_cols, HEAD), BF16)
    field1 = shaped((e_rows + 2, e_cols, HEAD), BF16)
    stats_shape = lambda n: shaped((n, 8, 2 * HEAD), F32)
    room = lambda a: pltpu.VMEM(a.shape, a.dtype)
    piece = shaped((bands, STAT_ROWS + t_rows * t_cols, HEAD), BF16)
    y2_shape = shaped((s_rows + 4, s_cols, HEAD), F32)
    coarse_call = pl.pallas_call(
        coarse_kernel,
        grid=(1,),
        out_shape=[y2_shape, piece],
        in_specs=[fixed(small), fixed(small), fixed(sixteenth), fixed(thirty), weight(2), weight(3)],
        out_specs=[fixed(y2_shape), fixed(piece)],
        scratch_shapes=[deep, deep],
        compiler_params=pltpu.CompilerParams(vmem_limit_bytes=20*1024*1024),
        name="coarse",
    )
    y2, pieces = coarse_call(
        small_before, small_after, sixteenth, thirty, first_weights, first_weights
    )
    got = everyone(pieces, ROWS)
    inside0, inside1 = pairs - 2, steps - 2
    c0, c1, inner0, inner1 = pl.pallas_call(
        inner_kernel,
        out_shape=[field0, field1, stats_shape(inside0), stats_shape(inside1)],
        in_specs=[ANY] * 4,
        out_specs=[ANY, ANY, VM, VM],
        scratch_shapes=[
            room(quarter), room(eighth), raw, raw, deep, deep, room(field0), room(field1),
            pltpu.SemaphoreType.DMA((2 * inside0 + inside1 + 3,)),
        ],
        compiler_params=params_of(),
        name="inner",
    )(quarter, eighth, first_weights, y2)
    up_small = jnp.asarray(doubling(t_cols), BF16)
    up_big = jnp.asarray(doubling(s_cols), BF16)
    up_cols = jnp.asarray(doubling(e_cols).T, BF16)
    narrow = pltpu.VMEM((4 * HEAD, 6 * HEAD), BF16)
    c0, c1, outer0, outer1, c4, c6, stats4, stats6, pieces = pl.pallas_call(
        between_kernel,
        out_shape=[
            field0, field1, stats_shape(2), stats_shape(2),
            field1, field1, stats_shape(steps), stats_shape(steps), shaped((bands, 8, HEAD), F32),
        ],
        in_specs=[SM, VM, ANY, ANY] + [VM] * 6 + [ANY] * 7,
        out_specs=[ANY, ANY, VM, VM, ANY, ANY, VM, VM, VM],
        input_output_aliases={15: 0, 16: 1},
        scratch_shapes=[
            room(y2), room(inner_weights), room(field1), room(field1),
            pltpu.VMEM((e_rows + 4, e_cols, HEAD), BF16),
            pltpu.VMEM((2 * t_rows * bands + 2, 2 * t_cols, HEAD), BF16),
            pltpu.VMEM((2 * t_rows * bands, 2 * t_cols, HEAD), F32),
            pltpu.VMEM((t_rows * bands, 8, 2 * HEAD), F32),
            narrow, narrow, narrow,
            pltpu.SemaphoreType.DMA((2 * steps + 14,)),
            pltpu.VMEM((6, q_cols, depth), BF16), pltpu.VMEM((4, e_cols, depth), BF16), room(big), room(big),
            raw, raw, deep, deep,
            pltpu.VMEM((4, q_cols, HEAD), BF16), pltpu.VMEM((4, e_cols, HEAD), BF16),
        ],
        compiler_params=params_of(),
        name="between",
    )(
        place, got, y2, inner_weights, norm_gain, norm_shift, up_small, up_big,
        inner0, inner1, quarter, eighth, big_before, big_after, first_weights, c0, c1,
    )
    got = everyone(pieces, ROWS)
    classes = class_weight.shape[1]
    class_t = jnp.pad(class_weight.T, ((0, SLOT - classes), (0, 0)))
    class_t3 = jnp.concatenate([class_t] * 3, axis=1)
    logits, pieces = pl.pallas_call(
        final_kernel,
        out_shape=[shaped((classes, q_rows, q_cols), BF16), shaped((devices, 2, HEAD), F32)],
        in_specs=[SM, SM] + [VM] * 16 + [ANY],
        out_specs=[VM, VM],
        scratch_shapes=[
            room(field0),
            pltpu.VMEM((e_rows + 2, SLOT, e_cols), F32),
            pltpu.VMEM((e_rows + 2, SLOT, q_cols), F32),
            pltpu.VMEM((q_cols // HEAD, q_rows * SLOT, HEAD), F32),
            pltpu.SemaphoreType.DMA((1,)),
        ],
        compiler_params=params_of(),
        name="final",
    )(
        place, class_bias, got, norm_gain, norm_shift, inner0, outer0, inner1, outer1, stats4, stats6,
        labels[0], class_t, class_t3, up_cols, c1, c4, c6, c0,
    )
    loss_total, valid_count = jnp.sum(everyone(pieces, EVERY), axis=(0, 2))
    mean_loss = loss_total / jnp.maximum(valid_count, 1.0)
    return (logits[None], mean_loss)


def solution(mesh):
    split = Mesh(mesh.devices.reshape(4, 2, 4, 4), ("batch_0", "batch_1", "rows_0", "rows_1"))
    in_specs = (
        P(BATCH, ROWS, None, None),
        P(BATCH, ROWS, None, None),
        P(BATCH, ROWS, None, None),
        P(BATCH, ROWS, None, None),
        P(BATCH, ROWS, None),
        P(),
        P(),
        P(),
        P(),
        P(),
        P(),
    )
    out_specs = (P(BATCH, None, ROWS, None), P())
    return jax.shard_map(device_step, mesh=split, in_specs=in_specs, out_specs=out_specs, check_vma=False)
```

```python
import jax
import jax.numpy as jnp
import numpy as np
from jax import lax
from jax.experimental import pallas as pl
from jax.experimental.pallas import tpu as pltpu
from jax.sharding import Mesh
from jax.sharding import PartitionSpec as P

GROUP = 4
HEAD = 128
ROWS = ("rows_0", "rows_1")
EVERY = ("batch_0", "batch_1", "rows_0", "rows_1")
BATCH = ("batch_0", "batch_1")
NORM_FLOOR = 0.05
SMALL = (3, 1)
BIG = (1, 2)
STAT_ROWS = 16
SLOT = 32
F32, BF16 = jnp.float32, jnp.bfloat16
VMEM_LIMIT = 60 * 1024 * 1024


def doubling(cols):
    matrix = np.zeros((2 * cols, cols), np.float32)
    for k in range(cols):
        matrix[2 * k, k] += 0.75
        matrix[2 * k, max(k - 1, 0)] += 0.25
        matrix[2 * k + 1, k] += 0.75
        matrix[2 * k + 1, min(k + 1, cols - 1)] += 0.25
    return matrix


def everyone(pieces, axes):
    return lax.all_to_all(pieces, axes, 0, 0)


def matmul(a, b):
    return jnp.dot(a, b, preferred_element_type=F32)


def matmul_t(a, b):
    return lax.dot_general(a, b, (((1,), (1,)), ((), ())), preferred_element_type=F32)


def fill_pair(w_ref, out_ref, depth):
    zero = jnp.zeros((depth, HEAD), BF16)
    for j in range(4):
        for across in range(3):
            rows = slice(j * depth, (j + 1) * depth)
            at = across * 2 * HEAD
            out_ref[rows, at : at + HEAD] = w_ref[j, across] if j < 3 else zero
            out_ref[rows, at + HEAD : at + 2 * HEAD] = w_ref[j - 1, across] if j else zero


def across_taps(z, width, cols):
    pixels = z.shape[0]
    index = lax.broadcasted_iota(jnp.int32, (pixels, width), 0) % cols
    left = jnp.where(index == 0, 0.0, pltpu.roll(z[:, :width], 1, 0))
    right = jnp.where(index == cols - 1, 0.0, pltpu.roll(z[:, 2 * width :], pixels - 1, 0))
    return z[:, width : 2 * width] + left + right


def conv_pair(rows, w_ref):
    return across_taps(matmul(jnp.concatenate(rows, axis=1), w_ref[...]), 2 * HEAD, rows[0].shape[0])


def fill_deep(w_ref, out_ref, depth):
    zero = jnp.zeros((depth, HEAD), BF16)
    for j in range(4):
        rows = slice(j * depth, (j + 1) * depth)
        if j < 3:
            out_ref[rows, :HEAD] = w_ref[j, 0]
            out_ref[rows, HEAD : 2 * HEAD] = w_ref[j, 1]
        out_ref[rows, 2 * HEAD : 3 * HEAD] = w_ref[j, 2] if j < 3 else zero
        out_ref[rows, 3 * HEAD :] = w_ref[j - 1, 2] if j else zero


def conv_deep(rows, w_ref):
    cols, depth = rows[0].shape
    wide = jnp.concatenate(rows, axis=1)
    stacked = jnp.concatenate([wide[:, : 3 * depth], wide[:, depth:]], axis=0)
    near = matmul(stacked, w_ref[: 3 * depth, : 2 * HEAD])
    far = matmul(wide, w_ref[:, 2 * HEAD :])
    taps = [jnp.concatenate([near[:cols, at : at + HEAD], near[cols:, at : at + HEAD]], axis=1) for at in (0, HEAD)]
    index = lax.broadcasted_iota(jnp.int32, far.shape, 0)
    left = jnp.where(index == 0, 0.0, pltpu.roll(taps[0], 1, 0))
    right = jnp.where(index == cols - 1, 0.0, pltpu.roll(far, cols - 1, 0))
    return taps[1] + left + right


def centre(y):
    total = jnp.sum(y, axis=0, keepdims=True)
    centred = y - total * (1.0 / y.shape[0])
    return total, jnp.sum(centred * centred, axis=0, keepdims=True), centred


def sums(y):
    return centre(y)[:2]


def merge(parts, pixels):
    total = sum(p[0] for p in parts)
    mean = total * (1.0 / (pixels * len(parts)))
    square = sum(p[1] + pixels * jnp.square(p[0] * (1.0 / pixels) - mean) for p in parts)
    return total, square


def halves(pair):
    total, square = pair
    return [(total[:, :HEAD], square[:, :HEAD]), (total[:, HEAD:], square[:, HEAD:])]


def group_sum(v):
    lane = lax.broadcasted_iota(jnp.int32, v.shape, 1)
    v = v + jnp.where(lane % 2 == 0, pltpu.roll(v, HEAD - 1, 1), pltpu.roll(v, 1, 1))
    return v + jnp.where(lane % 4 < 2, pltpu.roll(v, HEAD - 2, 1), pltpu.roll(v, 2, 1))


def normed(y, mean, factor, shift):
    return jnp.maximum((y - mean) * factor + shift, 0.0).astype(BF16)


def offset(total, pixels, norm):
    mean, factor, shift = norm
    return (total * (1.0 / pixels) - mean) * factor + shift


def lifted(centred, factor, at):
    return jnp.maximum(centred.astype(F32) * factor + at, 0.0).astype(BF16)


def split_rows(values):
    high = values.astype(BF16).astype(F32)
    rest = values - high
    middle = rest.astype(BF16).astype(F32)
    return [high, middle, rest - middle]


def edges_kernel(quarter, eighth, sixteenth, thirty, small_before, small_after, big_before, big_after, sems):
    copies = []
    groups = (
        (SMALL, (sixteenth, thirty), small_before, small_after),
        (BIG, (quarter, eighth), big_before, big_after),
    )
    for depths, feats, before, after in groups:
        at = 0
        for depth, feat in zip(depths, feats):
            rows, cols, _ = feat.shape
            for i in range(depth):
                spot = pl.ds(at, cols)
                copies.append((feat.at[rows - depth + i], before.at[spot]))
                copies.append((feat.at[i], after.at[spot]))
                at += cols
    started = [pltpu.make_async_copy(a, b, sems.at[i]) for i, (a, b) in enumerate(copies)]
    for copy in started:
        copy.start()
    for copy in started:
        copy.wait()


class Copies:
    def __init__(self, sems):
        self.sems, self.used = sems, 0

    def start(self, source, target):
        copy = pltpu.make_async_copy(source, target, self.sems.at[self.used])
        self.used += 1
        copy.start()
        return copy


def keep_pair(y, field, stats, index, pair):
    total, square, centred = centre(y)
    field[2 * pair] = centred[:, :HEAD].astype(BF16)
    field[2 * pair + 1] = centred[:, HEAD:].astype(BF16)
    stats[index, 0:1] = total
    stats[index, 1:2] = square


def inner_kernel(
    quarter, eighth, weights, _, c0_out, c1_out, stats0, stats1, x0, x1, w0, w1, deep0, deep1, c0, c1, sems
):
    copies = Copies(sems)
    rows0 = pl.ds(1, quarter.shape[0] - 2)
    waits1 = [copies.start(weights.at[1], w1), copies.start(eighth, x1)]
    waits0 = [copies.start(weights.at[0], w0), copies.start(quarter.at[rows0], x0.at[rows0])]
    out = []
    for wait in waits1:
        wait.wait()
    fill_deep(w1, deep1, 2 * HEAD)
    for i in range(stats1.shape[0]):
        p = i + 1
        keep_pair(conv_deep([x1[2 * i + j] for j in range(4)], deep1), c1, stats1, i, p)
        out.append(copies.start(c1.at[pl.ds(2 * p, 2)], c1_out.at[pl.ds(2 * p, 2)]))
    for wait in waits0:
        wait.wait()
    fill_deep(w0, deep0, 2 * HEAD)
    for i in range(stats0.shape[0]):
        p = i + 1
        keep_pair(conv_deep([x0[2 * i + 1 + j] for j in range(4)], deep0), c0, stats0, i, p)
        out.append(copies.start(c0.at[pl.ds(2 * p, 2)], c0_out.at[pl.ds(2 * p, 2)]))
    for copy in out:
        copy.wait()


class Outer:
    def __init__(self, copies, inputs, outputs, room):
        self.copies, self.outputs, self.room = copies, outputs, room
        quarter, eighth, before, after, weights = inputs
        x0, x1, low, high, w0, w1 = room[:6]
        self.q_rows, self.cols, _ = quarter.shape
        self.e_rows, self.e_cols, _ = eighth.shape
        pairs = (
            (weights.at[1], w1),
            (weights.at[0], w0),
            (before, low),
            (after, high),
            (eighth.at[pl.ds(0, 2)], x1.at[pl.ds(0, 2)]),
            (eighth.at[pl.ds(self.e_rows - 2, 2)], x1.at[pl.ds(2, 2)]),
            (quarter.at[pl.ds(0, 3)], x0.at[pl.ds(0, 3)]),
            (quarter.at[pl.ds(self.q_rows - 3, 3)], x0.at[pl.ds(3, 3)]),
        )
        self.waits = [copies.start(*pair) for pair in pairs]

    def work(self):
        for wait in self.waits:
            wait.wait()
        c0_out, c1_out, stats0, stats1 = self.outputs
        x0, x1, low, high, w0, w1, deep0, deep1, c0, c1 = self.room
        fill_deep(w1, deep1, 2 * HEAD)
        fill_deep(w0, deep0, 2 * HEAD)
        cols, e_cols = self.cols, self.e_cols
        for i in range(2):
            rows = [x0[3 * i + j] for j in range(3)]
            keep_pair(conv_deep(rows + [high[:cols]] if i else [low[:cols]] + rows, deep0), c0, stats0, i, i)
        for i in range(2):
            halo = high if i else low
            rows = [x1[2 * i + j] for j in range(2)]
            extra = [halo[cols + j * e_cols : cols + (j + 1) * e_cols] for j in range(2)]
            keep_pair(conv_deep(rows + extra if i else extra + rows, deep1), c1, stats1, i, i)
        out = []
        for i in range(2):
            spot = pl.ds(2 * i, 2)
            out.append(self.copies.start(c0.at[spot], c0_out.at[pl.ds(i * (self.q_rows - 2), 2)]))
            out.append(self.copies.start(c1.at[spot], c1_out.at[pl.ds(i * self.e_rows, 2)]))
        return out


def coarse_kernel(before, after, sixteenth, thirty, w2, w3, y2, pieces, wide2, wide3):
    depth = 2 * HEAD
    fill_deep(w2, wide2, depth)
    fill_deep(w3, wide3, depth)
    own, cols, _ = sixteenth.shape
    ring = SMALL[0]
    rows = [before[i * cols : (i + 1) * cols] for i in range(ring)]
    rows += [sixteenth[i] for i in range(own)]
    rows += [after[i * cols : (i + 1) * cols] for i in range(ring)]
    parts = []
    for p in range(y2.shape[0] // 2):
        out = conv_deep(rows[2 * p : 2 * p + 4], wide2)
        y2[2 * p] = out[:, :HEAD]
        y2[2 * p + 1] = out[:, HEAD:]
        if 0 < p < y2.shape[0] // 2 - 1:
            parts += halves(sums(out))
    at = ring * cols
    out = conv_deep([before[at:], thirty[0], thirty[1], after[at:]], wide3)
    total3, square3, coarse = centre(jnp.concatenate([out[:, :HEAD], out[:, HEAD:]], axis=0))
    coarse = coarse.astype(BF16)
    total, square = merge(parts, cols)
    values = jnp.concatenate([total, square, total3, square3], axis=0)
    head = jnp.concatenate(split_rows(values) + [jnp.zeros((4, HEAD), F32)], axis=0).astype(BF16)
    for i in range(pieces.shape[0]):
        pieces[i, :STAT_ROWS] = head
        pieces[i, STAT_ROWS:] = coarse


def between_kernel(
    place, got, y2_in, weights_in, gain, shift, up_small, up_big, inner0, inner1,
    quarter, eighth, before, after, first_weights, _, __,
    c0_out, c1_out, outer0, outer1, c4_out, c6_out, stats4, stats6, pieces,
    y2, weights, c4, c6, fine, coarse, field5, stats5, wide0, wide1, wide2, sems, *room,
):
    members = got.shape[0]
    position = place[0]
    first, last = position == 0, position == members - 1
    copies = Copies(sems)
    wait_w = copies.start(weights_in, weights)
    wait_y2 = copies.start(y2_in, y2)
    outer = Outer(
        copies, (quarter, eighth, before, after, first_weights), (c0_out, c1_out, outer0, outer1), room
    )
    out = []

    def merged_norm(each, pixels, layer):
        count = pixels * len(each) * GROUP
        mean = group_sum(jnp.broadcast_to(sum(p[0] for p in each), (8, HEAD)))[0:1] * (1.0 / count)
        square = sum(p[1] + pixels * jnp.square(p[0] * (1.0 / pixels) - mean) for p in each)
        var = group_sum(jnp.broadcast_to(square, (8, HEAD)))[0:1] * (1.0 / count)
        return mean, gain[layer : layer + 1] * lax.rsqrt(var + NORM_FLOOR), shift[layer : layer + 1]

    def up_conv(acts, wide, kept, kept_out, stats):
        count = len(acts)
        doubled = []
        for k in range(0, count, 2):
            both = matmul(up_big[...], jnp.concatenate([acts[k], acts[k + 1]], axis=1))
            doubled += [both[:, :HEAD], both[:, HEAD:]]
        lines = 2 * (count - 2)
        for k in range(1, count - 1):
            for half, other in ((0, k - 1), (1, k + 1)):
                line = 0.75 * doubled[k] + 0.25 * doubled[other]
                at = 2 * (k - 1) + half
                if at < 2:
                    line = jnp.where(first, 0.0, line)
                if at >= lines - 2:
                    line = jnp.where(last, 0.0, line)
                fine[at] = line.astype(BF16)
        own = []
        for p in range(lines // 2 - 1):
            keep_pair(conv_pair([fine[2 * p + j] for j in range(4)], wide), kept, stats, p, p)
            span = pl.ds(2 * p, 2)
            out.append(copies.start(kept.at[span], kept_out.at[span]))
            two = halves((stats[p, 0:1], stats[p, 1:2]))
            own += two[1:] if p == 0 else two[:1] if p == lines // 2 - 2 else two
        return merge(own, kept.shape[1])

    lines, cols = coarse.shape[0] - 2, coarse.shape[1]
    small = cols // 2
    blocks = [got[i, :STAT_ROWS].astype(F32) for i in range(members)]
    blocks = [b[0:4] + b[4:8] + b[8:12] for b in blocks]
    norm3 = merged_norm([(b[2:3], b[3:4]) for b in blocks], 2 * small, 3)
    doubled = []
    for i in range(members):
        a = lifted(got[i, STAT_ROWS:], norm3[1], offset(blocks[i][2:3], 2 * small, norm3))
        both = matmul(up_small[...], jnp.concatenate([a[:small], a[small:]], axis=1))
        doubled += [both[:, :HEAD], both[:, HEAD:]]
    coarse[0] = jnp.zeros((cols, HEAD), BF16)
    coarse[lines + 1] = jnp.zeros((cols, HEAD), BF16)
    for k in range(len(doubled)):
        for half, other in ((0, max(k - 1, 0)), (1, min(k + 1, len(doubled) - 1))):
            coarse[1 + 2 * k + half] = (0.75 * doubled[k] + 0.25 * doubled[other]).astype(BF16)
    wait_w.wait()
    for i, wide in enumerate((wide0, wide1, wide2)):
        fill_pair(weights.at[i], wide, HEAD)
    fold = 2

    def step(q, carry):
        base = q * (2 * fold)
        lhs = jnp.concatenate(
            [
                jnp.concatenate([coarse[base + 2 * i + j] for j in range(4)], axis=1)
                for i in range(fold)
            ],
            axis=0,
        )
        y = across_taps(matmul(lhs, wide1[...]), 2 * HEAD, cols)
        for i in range(fold):
            field5[base + 2 * i] = y[i * cols : (i + 1) * cols, :HEAD]
            field5[base + 2 * i + 1] = y[i * cols : (i + 1) * cols, HEAD:]
        total, square = sums(y)
        stats5[q, 0:1] = total
        stats5[q, 1:2] = square
        return carry

    lax.fori_loop(0, lines // (2 * fold), step, 0, unroll=True)
    out += outer.work()
    wait_y2.wait()
    norm2 = merged_norm([(b[0:1], b[1:2]) for b in blocks], y2.shape[1] * (y2.shape[0] - 4), 2)
    acts = [normed(y2[i], *norm2) for i in range(y2.shape[0])]
    count = len(acts)
    acts[1] = jnp.where(first, acts[2], acts[1])
    acts[count - 2] = jnp.where(last, acts[count - 3], acts[count - 2])
    merged4 = up_conv(acts, wide0, c4, c4_out, stats4)
    parts5 = []
    for q in range(lines // (2 * fold)):
        parts5 += halves((stats5[q, 0:1], stats5[q, 1:2]))
    norm5 = merged_norm(parts5, cols * fold, 5)
    band = lines // members
    acts = []
    for i in range(band + 4):
        at = jnp.clip(position * band + (i - 2), 0, lines - 1)
        acts.append(normed(field5[at], *norm5))
    merged6 = up_conv(acts, wide2, c6, c6_out, stats6)
    parts0, parts1 = [], []
    for stats in (inner0, outer0):
        for p in range(stats.shape[0]):
            parts0 += halves((stats[p, 0:1], stats[p, 1:2]))
    for p in range(inner1.shape[0]):
        parts1 += halves((inner1[p, 0:1], inner1[p, 1:2]))
    for p in range(2):
        parts1.append(halves((outer1[p, 0:1], outer1[p, 1:2]))[1 - p])
    eighth_cols = c4.shape[1]
    merged = [merge(parts0, 2 * eighth_cols), merge(parts1, eighth_cols), merged4, merged6]
    block = jnp.concatenate([m[0] for m in merged] + [m[1] for m in merged], axis=0)
    for i in range(members):
        pieces[i] = block
    for copy in out:
        copy.wait()


def final_kernel(
    place, bias, got, gain, shift, inner0, outer0, inner1, outer1, stats4, stats6, labels, class_t, class_t3, up_cols,
    c1, c4, c6, c0_in, logits, pieces, c0, lines, doubled, scores, sems,
):
    members = got.shape[0]
    copies = Copies(sems)
    rows = c0.shape[0]
    wait0 = copies.start(c0_in, c0)
    count = c4.shape[0]
    first, last = place[0] == 0, place[0] == members - 1
    row = lax.broadcasted_iota(jnp.int32, (4, HEAD), 0)
    own = float((count - 2) * c4.shape[1])
    pixels = jnp.where(row == 0, 4.0 * own, own)
    total = sum(got[i, 0:4] for i in range(members))
    mean = group_sum(total) / (pixels * (members * GROUP))
    square = sum(got[i, 4:8] + pixels * jnp.square(got[i, 0:4] / pixels - mean) for i in range(members))
    scale = lax.rsqrt(group_sum(square) / (pixels * (members * GROUP)) + NORM_FLOOR)
    norms = [
        (mean[j : j + 1], gain[layer : layer + 1] * scale[j : j + 1], shift[layer : layer + 1])
        for j, layer in enumerate((0, 1, 4, 6))
    ]

    def lift(field, r, total, norm):
        half = total[:, (r % 2) * HEAD : (r % 2 + 1) * HEAD]
        return lifted(field[r], norm[1], offset(half, field.shape[1], norm))

    def joined(inner, outer):
        pairs = [inner[p, 0:1] for p in range(inner.shape[0])]
        return [outer[0, 0:1]] + pairs + [outer[1, 0:1]]

    totals0, totals1 = joined(inner0, outer0), joined(inner1, outer1)
    for i in range(count):
        p = i // 2
        acts = [
            lift(c1, i, totals1[p], norms[1]),
            lift(c4, i, stats4[p, 0:1], norms[2]),
            lift(c6, i, stats6[p, 0:1], norms[3]),
        ]
        lines[i] = matmul_t(class_t3[...], jnp.concatenate(acts, axis=1))
    lines[0] = jnp.where(first, lines[1], lines[0])
    lines[count - 1] = jnp.where(last, lines[count - 2], lines[count - 1])
    for i in range(count):
        value = lines[i]
        high = value.astype(BF16)
        low = (value - high.astype(F32)).astype(BF16)
        both = matmul(jnp.concatenate([high, low], axis=0), up_cols[...])
        doubled[i] = both[:SLOT] + both[SLOT:]
    wait0.wait()
    for r in range(rows):
        p = r // 2
        value = matmul_t(class_t[...], lift(c0, r, totals0[p], norms[0]))
        value = value + (0.75 * doubled[p + 1] + 0.25 * doubled[p + 2 * (r % 2)])
        for i in range(scores.shape[0]):
            scores[i, r * SLOT : (r + 1) * SLOT] = value[:, i * HEAD : (i + 1) * HEAD]
    label_map = labels[...]
    exps = jnp.zeros(label_map.shape, F32)
    picked = jnp.zeros(label_map.shape, F32)
    for c in range(logits.shape[0]):
        tiles = [scores.at[i][pl.ds(c, rows, stride=SLOT), :] for i in range(scores.shape[0])]
        score = jnp.concatenate(tiles, axis=1) + bias[c]
        logits[c] = score.astype(BF16)
        exps = exps + jnp.exp(score)
        picked = picked + jnp.where(label_map == c, score, 0.0)
    usable = label_map != 255
    terms = jnp.where(usable, jnp.log(exps) - picked, 0.0)
    counts = jnp.where(usable, 1.0, 0.0)
    out = []
    for v in (terms, counts):
        v = jnp.sum(v, axis=0, keepdims=True)
        out.append(sum(v[:, i * HEAD : (i + 1) * HEAD] for i in range(v.shape[1] // HEAD)))
    lane = lax.broadcasted_iota(jnp.int32, out[0].shape, 1)
    folded = [v + pltpu.roll(v, HEAD // 2, 1) for v in out]
    both = jnp.where(lane < HEAD // 2, folded[0], folded[1])
    for i in range(pieces.shape[0]):
        pieces[i] = both


def params_of(**kw):
    return pltpu.CompilerParams(vmem_limit_bytes=VMEM_LIMIT, **kw)


def shaped(shape, dtype):
    return jax.ShapeDtypeStruct(shape, dtype)


VM = pl.BlockSpec(memory_space=pltpu.VMEM)
SM = pl.BlockSpec(memory_space=pltpu.SMEM)
ANY = pl.BlockSpec(memory_space=pl.ANY)


def device_step(
    feat_quarter,
    feat_eighth,
    feat_sixteenth,
    feat_thirty,
    labels,
    first_weights,
    inner_weights,
    norm_gain,
    norm_shift,
    class_weight,
    class_bias,
):
    position = lax.axis_index(ROWS)
    bands = lax.axis_size(ROWS)
    devices = bands * lax.axis_size(BATCH)
    place = position.astype(jnp.int32).reshape(1)
    up_pairs = [(i, i + 1) for i in range(bands - 1)]
    down_pairs = [(j, i) for i, j in up_pairs]
    feats = [feat_quarter[0], feat_eighth[0], feat_sixteenth[0], feat_thirty[0]]
    quarter, eighth, sixteenth, thirty = feats
    q_rows, q_cols, depth = quarter.shape
    e_rows, e_cols, _ = eighth.shape
    s_rows, s_cols, _ = sixteenth.shape
    t_rows, t_cols, _ = thirty.shape
    small = shaped((SMALL[0] * s_cols + SMALL[1] * t_cols, depth), BF16)
    big = shaped((BIG[0] * q_cols + BIG[1] * e_cols, depth), BF16)
    small_before, small_after, big_before, big_after = pl.pallas_call(
        edges_kernel,
        out_shape=[small, small, big, big],
        in_specs=[ANY] * 4,
        out_specs=[VM] * 4,
        scratch_shapes=[pltpu.SemaphoreType.DMA((2 * (sum(SMALL) + sum(BIG)),))],
        compiler_params=params_of(),
        name="edges",
    )(*feats)
    small_before = lax.ppermute(small_before, ROWS, up_pairs)
    small_after = lax.ppermute(small_after, ROWS, down_pairs)
    big_before = lax.ppermute(big_before, ROWS, up_pairs)
    big_after = lax.ppermute(big_after, ROWS, down_pairs)

    def fixed(a, *index):
        index = index or (0,) * len(a.shape)
        return pl.BlockSpec(a.shape, lambda i: index)

    def weight(level):
        return pl.BlockSpec((None,) + first_weights.shape[1:], lambda i: (level, 0, 0, 0, 0))

    deep = pltpu.VMEM((4 * depth, 4 * HEAD), BF16)
    raw = pltpu.VMEM(first_weights.shape[1:], BF16)
    pairs = q_rows // 2
    steps = e_rows // 2 + 1
    field0 = shaped((q_rows, q_cols, HEAD), BF16)
    field1 = shaped((e_rows + 2, e_cols, HEAD), BF16)
    stats_shape = lambda n: shaped((n, 8, 2 * HEAD), F32)
    room = lambda a: pltpu.VMEM(a.shape, a.dtype)
    piece = shaped((bands, STAT_ROWS + t_rows * t_cols, HEAD), BF16)
    y2_shape = shaped((s_rows + 4, s_cols, HEAD), F32)
    coarse_call = pl.pallas_call(
        coarse_kernel,
        grid=(1,),
        out_shape=[y2_shape, piece],
        in_specs=[fixed(small), fixed(small), fixed(sixteenth), fixed(thirty), weight(2), weight(3)],
        out_specs=[fixed(y2_shape), fixed(piece)],
        scratch_shapes=[deep, deep],
        compiler_params=pltpu.CompilerParams(vmem_limit_bytes=20*1024*1024),
        name="coarse",
    )
    y2, pieces = coarse_call(
        small_before, small_after, sixteenth, thirty, first_weights, first_weights
    )
    got = everyone(pieces, ROWS)
    inside0, inside1 = pairs - 2, steps - 2
    c0, c1, inner0, inner1 = pl.pallas_call(
        inner_kernel,
        out_shape=[field0, field1, stats_shape(inside0), stats_shape(inside1)],
        in_specs=[ANY] * 4,
        out_specs=[ANY, ANY, VM, VM],
        scratch_shapes=[
            room(quarter), room(eighth), raw, raw, deep, deep, room(field0), room(field1),
            pltpu.SemaphoreType.DMA((2 * inside0 + inside1 + 3,)),
        ],
        compiler_params=params_of(),
        name="inner",
    )(quarter, eighth, first_weights, y2)
    up_small = jnp.asarray(doubling(t_cols), BF16)
    up_big = jnp.asarray(doubling(s_cols), BF16)
    up_cols = jnp.asarray(doubling(e_cols).T, BF16)
    narrow = pltpu.VMEM((4 * HEAD, 6 * HEAD), BF16)
    c0, c1, outer0, outer1, c4, c6, stats4, stats6, pieces = pl.pallas_call(
        between_kernel,
        out_shape=[
            field0, field1, stats_shape(2), stats_shape(2),
            field1, field1, stats_shape(steps), stats_shape(steps), shaped((bands, 8, HEAD), F32),
        ],
        in_specs=[SM, VM, ANY, ANY] + [VM] * 6 + [ANY] * 7,
        out_specs=[ANY, ANY, VM, VM, ANY, ANY, VM, VM, VM],
        input_output_aliases={15: 0, 16: 1},
        scratch_shapes=[
            room(y2), room(inner_weights), room(field1), room(field1),
            pltpu.VMEM((e_rows + 4, e_cols, HEAD), BF16),
            pltpu.VMEM((2 * t_rows * bands + 2, 2 * t_cols, HEAD), BF16),
            pltpu.VMEM((2 * t_rows * bands, 2 * t_cols, HEAD), F32),
            pltpu.VMEM((t_rows * bands, 8, 2 * HEAD), F32),
            narrow, narrow, narrow,
            pltpu.SemaphoreType.DMA((2 * steps + 14,)),
            pltpu.VMEM((6, q_cols, depth), BF16), pltpu.VMEM((4, e_cols, depth), BF16), room(big), room(big),
            raw, raw, deep, deep,
            pltpu.VMEM((4, q_cols, HEAD), BF16), pltpu.VMEM((4, e_cols, HEAD), BF16),
        ],
        compiler_params=params_of(),
        name="between",
    )(
        place, got, y2, inner_weights, norm_gain, norm_shift, up_small, up_big,
        inner0, inner1, quarter, eighth, big_before, big_after, first_weights, c0, c1,
    )
    got = everyone(pieces, ROWS)
    classes = class_weight.shape[1]
    class_t = jnp.pad(class_weight.T, ((0, SLOT - classes), (0, 0)))
    class_t3 = jnp.concatenate([class_t] * 3, axis=1)
    logits, pieces = pl.pallas_call(
        final_kernel,
        out_shape=[shaped((classes, q_rows, q_cols), BF16), shaped((devices, 1, HEAD), F32)],
        in_specs=[SM, SM] + [VM] * 16 + [ANY],
        out_specs=[VM, VM],
        scratch_shapes=[
            room(field0),
            pltpu.VMEM((e_rows + 2, SLOT, e_cols), F32),
            pltpu.VMEM((e_rows + 2, SLOT, q_cols), F32),
            pltpu.VMEM((q_cols // HEAD, q_rows * SLOT, HEAD), F32),
            pltpu.SemaphoreType.DMA((1,)),
        ],
        compiler_params=params_of(),
        name="final",
    )(
        place, class_bias, got, norm_gain, norm_shift, inner0, outer0, inner1, outer1, stats4, stats6,
        labels[0], class_t, class_t3, up_cols, c1, c4, c6, c0,
    )
    sums_of = jnp.sum(everyone(pieces, EVERY), axis=(0, 1))
    loss_total, valid_count = jnp.sum(sums_of[: HEAD // 2]), jnp.sum(sums_of[HEAD // 2 :])
    mean_loss = loss_total / jnp.maximum(valid_count, 1.0)
    return (logits[None], mean_loss)


def solution(mesh):
    split = Mesh(mesh.devices.reshape(4, 2, 4, 4), ("batch_0", "batch_1", "rows_0", "rows_1"))
    in_specs = (
        P(BATCH, ROWS, None, None),
        P(BATCH, ROWS, None, None),
        P(BATCH, ROWS, None, None),
        P(BATCH, ROWS, None, None),
        P(BATCH, ROWS, None),
        P(),
        P(),
        P(),
        P(),
        P(),
        P(),
    )
    out_specs = (P(BATCH, None, ROWS, None), P())
    return jax.shard_map(device_step, mesh=split, in_specs=in_specs, out_specs=out_specs, check_vma=False)
```
